32 devices in a mesh: gx: 4 (over z), gy: 8 (over y, x, core).
Axes of the slice: x: 2, y: 2, z: 4, core: 2. Of those that a mesh axis runs over, the one named last changes fastest.
Arguments:
- coordinates: float32 [3, 65536], P(None, ('gx', 'gy')), may hold values from 0 to 1
- rhs: float32 [16, 65536], P(None, ('gx', 'gy')), may hold values from -70 to 70
- leaf_order: int32 [32, 2048], P(('gx', 'gy')), may hold values from 0 to 2047, each once within a row
- leaf_sizes: int32 [32], P(('gx', 'gy')), may hold values from 1 to 2048, 49152 in all
- inverse_scales: float32 [3], replicated, may hold values from 12 to 30
- noise_var: float32 [1], replicated, may hold values from 0.3 to 1
- u_factors: float32 [5, 64, 65536], P(None, None, ('gx', 'gy')), may hold values from -0.375 to 0.375
- v_factors: float32 [5, 64, 65536], P(None, None, ('gx', 'gy')), may hold values from -1 to 1
Outputs:
- solution: float32 [16, 65536], P(None, ('gx', 'gy'))
The draws below stay inside these ranges and needn't reach their ends.
Inputs may be any that keep to these rules, and one draw needn't show every extreme that they name: `leaf_sizes`: each leaf's live points stand first in leaf order.
All inputs are finite; a program needn't handle non-finite values. No bound on the sum of `leaf_sizes` on one device may be relied on, other than what follows from the above.
Results may differ from the reference program's by a relative error of at most 0.0001.
Values sent between devices are 32-bit elements; how exact they have to be, the bound alone decides.
A program may use at most 128 MiB of HBM per device.

```python
import math
import jax
import jax.numpy as jnp
import numpy as np
from jax import lax

LEAF = 2048
RANK = 64
VECTORS = 16
ITERS = 3
LEVELS = 5
LEAVES = 32
POINTS = 65536


def draw_v_factors(key, part):
    key_values = jax.random.fold_in(key, 11)
    level_ids = jnp.arange(LEVELS, dtype=jnp.float32)
    level_scale = 1.0 / jnp.sqrt(LEAF * 2.0 ** level_ids)
    values = jnp.clip(jax.random.normal(key_values, (LEVELS, RANK, POINTS), jnp.float32), -5.0, 5.0)
    return values * level_scale[:, None, None]


def draw_rhs(key, part):
    key_main = jax.random.fold_in(key, 21)
    key_column = jax.random.fold_in(key, 22)
    key_row = jax.random.fold_in(key, 23)
    position = jnp.arange(POINTS, dtype=jnp.float32) / POINTS
    column_scale = jnp.exp(jax.random.uniform(key_column, (1, POINTS), jnp.float32, 0.0, math.log(2.5)))
    row_scale = jnp.exp(jax.random.uniform(key_row, (VECTORS, 1), jnp.float32, math.log(1.0 / 3.0), math.log(10.0 / 3.0)))
    base = jnp.clip(jax.random.normal(key_main, (VECTORS, POINTS), jnp.float32), -4.0, 4.0)
    base = base * 0.5 * jnp.exp(math.log(3.0) * position)[None, :]
    return base * column_scale * row_scale


def levels(rng, shape, shards, low, high):
    def one(dim, parts):
        draws = jax.random.uniform(jax.random.fold_in(jax.random.fold_in(rng, 6), dim), (parts,), jnp.float32, low / len(shards), high / len(shards))
        return jnp.repeat(jnp.exp(draws), shape[dim] // parts).reshape((-1,) + (1,) * (len(shape) - dim - 1))

    gain = one(*shards[0])
    for cut in shards[1:]:
        gain = gain * one(*cut)
    return gain


def profile(amount, total, bound, slope):
    weights = [(1 << 20) // math.isqrt(rank ** slope) + 1 for rank in range(2, amount + 1)]
    rest, counts = total - bound - (amount - 1), [1] * (amount - 1)
    while rest > 0:
        movable = [i for i in range(amount - 1) if counts[i] < bound]
        whole, left = sum([weights[i] for i in movable]), rest
        for i in movable:
            addition = min(bound - counts[i], max(1, left * weights[i] // whole), rest)
            counts[i] = counts[i] + addition
            rest = rest - addition
    return np.array([bound] + counts)


def ragged_sizes(stream_key, amount, total, reach, skew):
    if amount == 2:
        one = jax.random.randint(stream_key, (), max(1, total - reach), min(reach, total - 1) + 1)
        return jnp.stack([one, total - one])
    sizes = jnp.asarray(profile(amount, total, reach, skew), jnp.int32)
    couples = (amount - 1) // 2
    donor, taker = sizes[1:1 + 2 * couples:2], sizes[2:2 + 2 * couples:2]
    room = jnp.minimum(donor - 1, reach - taker)
    shifted = jax.random.randint(jax.random.fold_in(stream_key, 1), (couples,), 0, 1 << 20) % (room + 1)
    sizes = sizes.at[1:1 + 2 * couples:2].set(donor - shifted).at[2:2 + 2 * couples:2].set(taker + shifted)
    return sizes[jax.random.permutation(jax.random.fold_in(stream_key, 2), amount)]


def scatter_about(rng, extent, width, bound, cuts=(), kind=jnp.bfloat16):
    values = jax.random.normal(rng, extent, jnp.float32) * width
    if len(cuts) > 0:
        values = levels(rng, extent, cuts, -0.22, 0.18) * values
    return jnp.clip(values, min=-bound, max=bound).astype(kind)


def setup_inputs(seed: int = 0) -> dict:
    splits = jax.random.split(jax.random.key(seed), 9)
    return {
        "coordinates": jnp.clip(1.0 * jax.random.uniform(splits[0], (3, POINTS), jnp.float32) ** levels(splits[0], (3, POINTS), ((1, 32),), -0.2, 0.2), 0.0, 1.0),
        "rhs": draw_rhs(jax.random.fold_in(splits[8], 71), 0),
        "leaf_order": jax.vmap(lambda own: jax.random.permutation(own, LEAF))(jax.random.split(splits[2], LEAVES)).reshape((LEAVES, LEAF)).astype(jnp.int32),
        "leaf_sizes": ragged_sizes(splits[3], LEAVES, LEAVES * LEAF * 3 // 4, LEAF, 1).astype(jnp.int32),
        "inverse_scales": jnp.clip(jnp.exp(jax.random.uniform(splits[4], (3,), jnp.float32, math.log(12.0), math.log(30.0))), 12.0, 30.0),
        "noise_var": jnp.clip(jnp.exp(jax.random.uniform(splits[5], (1,), jnp.float32, math.log(0.3), math.log(1.0))), 0.3, 1.0),
        "u_factors": scatter_about(splits[6], (LEVELS, RANK, POINTS), (4 * RANK) ** -0.5, 0.375, ((2, 32),), jnp.float32),
        "v_factors": draw_v_factors(jax.random.fold_in(splits[8], 71), 0),
    }


epsilon = 1e-06
sqrt_three = math.sqrt(3.0)
highest = lax.Precision.HIGHEST

def build_kernel(scaled):
    width_all = scaled.shape[1]
    block_rows = min(512, width_all)
    pieces = []
    for start_row in range(0, width_all, block_rows):
        row_points = scaled[:, start_row:start_row + block_rows]
        differ = row_points[:, :, None] - scaled[:, None, :]
        distance = jnp.sqrt(lax.optimization_barrier(jnp.sum(differ * differ, axis=0)))
        pieces.append((1.0 + sqrt_three * distance) * jnp.exp(-sqrt_three * distance))
    return jnp.concatenate(pieces, axis=0)

def least_squares(columns, beta):
    count_cols = len(columns)
    cosines = []
    sines = []
    target = [beta] + [jnp.zeros_like(beta)] * count_cols
    upper = []
    for column_idx in range(count_cols):
        entries = list(columns[column_idx])
        for row_idx in range(column_idx):
            first_val = entries[row_idx]
            second_val = entries[row_idx + 1]
            entries[row_idx] = cosines[row_idx] * first_val + sines[row_idx] * second_val
            entries[row_idx + 1] = -sines[row_idx] * first_val + cosines[row_idx] * second_val
        first_val = entries[column_idx]
        second_val = entries[column_idx + 1]
        radius = jnp.sqrt(first_val * first_val + second_val * second_val)
        cosines.append(first_val / radius)
        sines.append(second_val / radius)
        entries[column_idx] = radius
        carried = target[column_idx]
        target[column_idx] = cosines[column_idx] * carried
        target[column_idx + 1] = -sines[column_idx] * carried
        upper.append(entries[:column_idx + 1])
    weights = [None] * count_cols
    for column_idx in reversed(range(count_cols)):
        accum = target[column_idx]
        for later_idx in range(column_idx + 1, count_cols):
            accum = accum - upper[later_idx][column_idx] * weights[later_idx]
        weights[column_idx] = accum / upper[column_idx][column_idx]
    return weights

def reference(coordinates, rhs, leaf_order, leaf_sizes, inverse_scales, noise_var, u_factors, v_factors):
    num_leaves = leaf_order.shape[0]
    leaf_len = leaf_order.shape[1]
    num_vectors = rhs.shape[0]
    num_levels = u_factors.shape[0]
    num_rank = u_factors.shape[1]
    num_points = num_leaves * leaf_len
    points = jnp.take_along_axis(coordinates.reshape(3, num_leaves, leaf_len), leaf_order[None], axis=2)
    scaled = points * inverse_scales[:, None, None]
    ordered = jnp.take_along_axis(rhs.reshape(num_vectors, num_leaves, leaf_len), leaf_order[None], axis=2)
    live_mask = (jnp.arange(leaf_len, dtype=jnp.int32)[None, :] < leaf_sizes[:, None]).astype(jnp.float32)
    scaled_leaves = jnp.moveaxis(scaled, 1, 0)

    def dense_part(vector):

        def one_leaf(pair):
            leaf_scaled, leaf_vector = pair
            kernel = build_kernel(leaf_scaled)
            return jnp.dot(leaf_vector, kernel, precision=highest)
        result = lax.map(one_leaf, (scaled_leaves, jnp.moveaxis(vector, 1, 0)))
        return jnp.moveaxis(result, 0, 1)

    def low_part(vector):
        flat = vector.reshape(num_vectors, num_points)
        total = jnp.zeros((num_vectors, num_leaves, leaf_len), jnp.float32)
        for level in range(num_levels):
            nodes = num_leaves >> level
            node_len = leaf_len << level
            right_fac = v_factors[level].reshape(num_rank, nodes, node_len)
            coef = jnp.einsum('rnp,knp->nrk', right_fac, flat.reshape(num_vectors, nodes, node_len), precision=highest)
            sibling = coef.reshape(nodes // 2, 2, num_rank, num_vectors)[:, ::-1].reshape(nodes, num_rank, num_vectors)
            left_fac = u_factors[level].reshape(num_rank, nodes, node_len)
            total = total + jnp.einsum('rnp,nrk->knp', left_fac, sibling, precision=highest).reshape(num_vectors, num_leaves, leaf_len)
        return total

    def operate(vector):
        return live_mask[None] * (dense_part(vector) + noise_var[0] * vector + low_part(vector))
    start = live_mask[None] * ordered
    beta = jnp.sqrt(lax.optimization_barrier(jnp.sum(start * start, axis=(1, 2))) + epsilon)
    basis = [start / beta[:, None, None]]
    columns = []
    for step_idx in range(ITERS):
        image = operate(basis[step_idx])
        column = [lax.optimization_barrier(jnp.sum(basis[row_idx] * image, axis=(1, 2))) for row_idx in range(step_idx + 1)]
        for row_idx in range(step_idx + 1):
            image = image - column[row_idx][:, None, None] * basis[row_idx]
        length = jnp.sqrt(lax.optimization_barrier(jnp.sum(image * image, axis=(1, 2))) + epsilon)
        column.append(length)
        columns.append(column)
        if step_idx + 1 < ITERS:
            basis.append(image / length[:, None, None])
    weights = least_squares(columns, beta)
    solved = weights[0][:, None, None] * basis[0]
    for step_idx in range(1, ITERS):
        solved = solved + weights[step_idx][:, None, None] * basis[step_idx]
    leaf_rows = jnp.arange(num_leaves, dtype=jnp.int32)[:, None]
    placed = jnp.zeros((num_vectors, num_leaves, leaf_len), jnp.float32).at[:, leaf_rows, leaf_order].set(solved)
    return placed.reshape(num_vectors, num_points)
```

```python
import contextlib
import functools
import math

import jax
import jax.numpy as jnp
from jax import lax
from jax.experimental import pallas as pl
from jax.experimental.pallas import tpu as pltpu
from jax.sharding import PartitionSpec as P

ITERS = 3

epsilon = 1e-06
sqrt_three = math.sqrt(3.0)
log2_e = math.log2(math.e)
MESH = pl.DeviceIdType.MESH
f32 = jnp.float32
bf16 = jnp.bfloat16
NN = (((1,), (0,)), ((), ()))
NT = (((1,), (1,)), ((), ()))


def least_squares(columns, beta):
    count_cols = len(columns)
    cosines = []
    sines = []
    target = [beta] + [jnp.zeros_like(beta)] * count_cols
    upper = []
    for column_idx in range(count_cols):
        entries = list(columns[column_idx])
        for row_idx in range(column_idx):
            first_val = entries[row_idx]
            second_val = entries[row_idx + 1]
            entries[row_idx] = cosines[row_idx] * first_val + sines[row_idx] * second_val
            entries[row_idx + 1] = -sines[row_idx] * first_val + cosines[row_idx] * second_val
        first_val = entries[column_idx]
        second_val = entries[column_idx + 1]
        radius = jnp.sqrt(first_val * first_val + second_val * second_val)
        cosines.append(first_val / radius)
        sines.append(second_val / radius)
        entries[column_idx] = radius
        carried = target[column_idx]
        target[column_idx] = cosines[column_idx] * carried
        target[column_idx + 1] = -sines[column_idx] * carried
        upper.append(entries[: column_idx + 1])
    weights = [None] * count_cols
    for column_idx in reversed(range(count_cols)):
        accum = target[column_idx]
        for later_idx in range(column_idx + 1, count_cols):
            accum = accum - upper[later_idx][column_idx] * weights[later_idx]
        weights[column_idx] = accum / upper[column_idx][column_idx]
    return weights


def flipped(index, bits):
    result = index
    place = 1
    while place <= bits:
        if bits & place:
            result = result + place * (1 - 2 * lax.rem(lax.div(index, place), 2))
        place *= 2
    return result


def split2(value):
    high = value.astype(bf16)
    low = (value - high.astype(f32)).astype(bf16)
    return high, low


def split3(value):
    high = value.astype(bf16)
    rest = value - high.astype(f32)
    mid = rest.astype(bf16)
    low = (rest - mid.astype(f32)).astype(bf16)
    return high, mid, low


@contextlib.contextmanager
def phase(name):
    pl.delay(1)
    with jax.named_scope(name):
        yield
    pl.delay(1)


def dot(left, right, dims=NN):
    return lax.dot_general(left, right, dims, preferred_element_type=f32)


def fused(
    size_gx, size_gy,
    coords_ref, rhs_ref, order_ref, sizes_ref, inv_ref, noise_ref, u_hbm, v_hbm,
    out_ref,
    near_hi, near_lo, pick_ref, left_ref, right_ref, u_raw, v_raw, u_hi, u_lo, v_hi, v_lo,
    basis_ref, image_ref,
    send_part, recv_low, recv_high, send_node, recv_node,
    send_dots, recv_dots,
    load_sem,
    part_s, part_r, node_s, node_r, dots_s, dots_r,
):
    me_x = lax.axis_index("gx")
    me_y = lax.axis_index("gy")
    levels_low = size_gy.bit_length() - 1
    levels_high = size_gx.bit_length() - 1
    nv, leaf_len = rhs_ref.shape
    num_dims = coords_ref.shape[0]
    num_levels, num_rank = u_raw.shape[0], u_raw.shape[1]
    half = nv // 2
    lanes = 2 * num_rank
    size_all = size_gx * size_gy

    u_load = pltpu.make_async_copy(u_hbm, u_raw, load_sem.at[0])
    v_load = pltpu.make_async_copy(v_hbm, v_raw, load_sem.at[1])
    v_load.start()
    u_load.start()

    peers = [
        (flipped(me_x, apart // size_gy), flipped(me_y, apart % size_gy)) for apart in range(size_all)
    ]
    barrier = pltpu.get_barrier_semaphore()
    for apart in range(1, size_all):
        pl.semaphore_signal(barrier, inc=1, device_id=peers[apart], device_id_type=MESH)

    def send(src, dst, sems, semr, device):
        copy = pltpu.make_async_remote_copy(
            src_ref=src, dst_ref=dst, send_sem=sems, recv_sem=semr,
            device_id=device, device_id_type=MESH,
        )
        copy.start()

    def landed(block, sem):
        pltpu.make_async_copy(block, block, sem).wait()

    live = jnp.where(
        lax.broadcasted_iota(jnp.int32, (1, leaf_len), 1) < sizes_ref[0], 1.0, 0.0
    ).astype(f32)

    width = 256
    groups = leaf_len // width
    order = order_ref[...]
    outer = lax.div(order, width)
    inner = order - outer * width
    with phase("onehot"):
        pick_ref[...] = jnp.where(
            lax.broadcasted_iota(jnp.int32, (width, leaf_len), 0) == inner, 1.0, 0.0
        ).astype(bf16)
    def gather(stack, pieces):
        rows = stack.shape[0] // pieces
        stacked = jnp.concatenate([stack[:, g * width : (g + 1) * width] for g in range(groups)], axis=0)
        blocks = []
        for start_col in range(0, leaf_len, 512):
            cols = slice(start_col, start_col + 512)
            got = dot(stacked, pick_ref[:, cols])
            total = jnp.zeros((rows, 512), f32)
            for g in range(groups):
                term = None
                for piece in range(pieces):
                    base = (g * pieces + piece) * rows
                    term = got[base : base + rows] if term is None else term + got[base : base + rows]
                total = jnp.where(outer[:, cols] == g, term, total)
            blocks.append(total)
        return jnp.concatenate(blocks, axis=1)

    with phase("gather_rhs"):
        basis_ref[0] = live * gather(jnp.concatenate(split3(rhs_ref[...]), axis=0), 3)

    padded = v_hi.shape[0]
    used = num_levels * num_rank

    def prepare(raw, hi, lo):
        for level in range(num_levels):
            first, second = split2(raw[level])
            hi[level * num_rank : (level + 1) * num_rank, :] = first
            lo[level * num_rank : (level + 1) * num_rank, :] = second
        if padded > used:
            hi[used:, :] = jnp.zeros((padded - used, leaf_len), bf16)
            lo[used:, :] = jnp.zeros((padded - used, leaf_len), bf16)

    lane = lax.broadcasted_iota(jnp.int32, (half, lanes), 1)
    left_side = lane < num_rank

    def swap(value):
        return pltpu.roll(value, num_rank, 1)

    def send_partials(it, coef):
        for level in range(num_levels):
            block = coef[:, (level // 2) * lanes : (level // 2 + 1) * lanes]
            top, bottom = block[:half], block[half:]
            if level % 2 == 0:
                tile = jnp.where(left_side, top, swap(bottom))
            else:
                tile = jnp.where(left_side, swap(top), bottom)
            send_part[it, level] = tile
        for apart in range(1, size_gy):
            send(
                send_part.at[it, pl.ds(levels_low, levels_high)], recv_high.at[it, apart],
                part_s.at[it, 1], part_r.at[it, 1], peers[apart],
            )
        for apart in range(1, size_gy):
            send(
                send_part.at[it, apart.bit_length() - 1], recv_low.at[it, apart],
                part_s.at[it, 0], part_r.at[it, 0], peers[apart],
            )

    def others(ref, it):
        return ref.at[it, pl.ds(1, ref.shape[1] - 1)]

    def send_nodes(it):
        with phase(f"wait_parts{it}"):
            landed(others(recv_high, it), part_r.at[it, 1])
        total = send_part[it, levels_low:num_levels]
        for apart in range(1, size_gy):
            total = total + recv_high[it, apart]
        send_node[it] = total
        for apart in range(1, size_gx):
            send(
                send_node.at[it, apart.bit_length() - 1], recv_node.at[it, apart],
                node_s.at[it], node_r.at[it], peers[apart * size_gy],
            )

    def siblings(it):
        with phase(f"wait_nodes{it}"):
            landed(others(recv_low, it), part_r.at[it, 0])
            landed(others(recv_node, it), node_r.at[it])
        tiles = []
        for count, source in ((levels_low, recv_low), (levels_high, recv_node)):
            for level in range(count):
                total = source[it, 2**level]
                for apart in range(2**level + 1, 2 ** (level + 1)):
                    total = total + source[it, apart]
                tiles.append(total)
        if len(tiles) % 2:
            tiles.append(jnp.zeros_like(tiles[0]))
        blocks = []
        for pair in range(len(tiles) // 2):
            even, odd = tiles[2 * pair], tiles[2 * pair + 1]
            top = jnp.where(left_side, even, swap(odd))
            bottom = jnp.where(left_side, swap(even), odd)
            blocks.append(jnp.concatenate([top, bottom], axis=0))
        return jnp.concatenate(blocks, axis=1)

    slots = lanes // nv
    row16 = lax.broadcasted_iota(jnp.int32, (nv, lanes), 0)
    slot16 = lax.broadcasted_iota(jnp.int32, (nv, lanes), 1) - row16 * slots

    def send_sums(it, values):
        block = jnp.zeros((nv, lanes), f32)
        for idx, value in enumerate(values):
            block = jnp.where(slot16 == idx, value, block)
        send_dots[it] = jnp.sum(block, axis=0, keepdims=True)
        for apart in range(1, size_all):
            send(
                send_dots.at[it], recv_dots.at[it, apart],
                dots_s.at[it], dots_r.at[it], peers[apart],
            )

    def read_sums(it, count):
        with phase(f"wait_sums{it}"):
            landed(others(recv_dots, it), dots_r.at[it])
        terms = [send_dots[it]] + [recv_dots[it, apart] for apart in range(1, size_all)]
        while len(terms) > 1:
            terms = [terms[i] + terms[i + 1] for i in range(0, len(terms), 2)]
        return [
            jnp.sum(jnp.where(slot16 == idx, terms[0], 0.0), axis=1, keepdims=True)
            for idx in range(count)
        ]

    chunk = min(256, leaf_len)

    def near_columns(both, first, begin, end):
        for low in range(begin, end, chunk):
            high = low + chunk
            cols = slice(low, high)
            wide = dot(both[:, :high], near_hi[:high, cols])
            rest = dot(first[:, :high], near_lo[:high, cols])
            if high < leaf_len:
                wide = wide + dot(both[:, high:], near_hi[cols, high:], NT)
                rest = rest + dot(first[:, high:], near_lo[cols, high:], NT)
            image_ref[:, cols] = wide[:nv] + wide[nv:] + rest

    strip = min(128, chunk)

    def fill_near(both, first, begin, end):
        for low in range(begin, end, chunk):
            high = low + chunk
            cols = slice(low, high)
            for base in range(0, high, strip):
                rows = slice(base, base + strip)
                square = dot(left_ref[rows, :], right_ref[:, cols])
                square = jnp.maximum(square, 1e-30)
                distance = square * lax.rsqrt(square)
                value = (1.0 + distance) * jnp.exp2(distance * (-log2_e))
                hi, lo = split2(value)
                near_hi[rows, cols] = hi
                near_lo[rows, cols] = lo
            wide = dot(both[:, :high], near_hi[:high, cols])
            image_ref[:, cols] = wide[:nv] + wide[nv:] + dot(first[:, :high], near_lo[:high, cols])
            if low:
                wide = dot(both[:, cols], near_hi[:low, cols], NT)
                rest = dot(first[:, cols], near_lo[:low, cols], NT)
                image_ref[:, :low] += wide[:nv] + wide[nv:] + rest

    def prepare_points():
        with phase("gather_pos"):
            coords = jnp.concatenate([coords_ref[...], jnp.zeros((16 - num_dims, leaf_len), f32)], axis=0)
            gathered = gather(jnp.concatenate(split3(coords), axis=0), 3)[:8]
        row8 = lax.broadcasted_iota(jnp.int32, (8, 1), 0)
        with phase("place"):
            scale = jnp.zeros((8, 1), f32)
            for dim in range(num_dims):
                scale = jnp.where(row8 == dim, inv_ref[dim] * sqrt_three, scale)
            place = (gathered - 0.5) * scale
            coarse = jnp.round(place * 4.0) * 0.25
            fine_hi, fine_lo = split2(place - coarse)
            fine_hi, fine_lo = fine_hi.astype(f32), fine_lo.astype(f32)
            fine = fine_hi + fine_lo
            whole_norm = jnp.sum(coarse * coarse, axis=0, keepdims=True)
            rest_norm = jnp.sum(fine * (2.0 * coarse + fine), axis=0, keepdims=True)
        def rows_of(values):
            block = jnp.zeros((8, leaf_len), f32)
            for idx, value in enumerate(values):
                block = jnp.where(row8 == idx, value, block)
            return block

        with phase("lr"):
            norms = [part.astype(f32) for part in split2(whole_norm)]
            rests = [part.astype(f32) for part in split3(rest_norm)]
            ones = [1.0] * 3
            pairs = [
                (-2.0 * coarse, coarse),
                (rows_of(norms + ones[:2]), rows_of(ones[:2] + norms)),
                (rows_of(rests + ones), rows_of(ones + rests)),
                (-2.0 * coarse, fine_hi),
                (-2.0 * coarse, fine_lo),
                (fine_hi, -2.0 * coarse),
                (fine_lo, -2.0 * coarse),
                (fine_hi, -2.0 * fine_hi),
                (fine_hi, -2.0 * fine_lo),
                (fine_lo, -2.0 * fine_hi),
            ]
            blank = jnp.zeros((128 - 8 * len(pairs), leaf_len), f32)
            left_ref[...] = jnp.concatenate([pair[0] for pair in pairs] + [blank], axis=0).T.astype(bf16)
            right_ref[...] = jnp.concatenate([pair[1] for pair in pairs] + [blank], axis=0).astype(bf16)

    def operate(it, vector, meanwhile):
        first, second = split2(vector)
        both = jnp.concatenate([first, second], axis=0)
        if it == 0:
            with phase("wait_v"):
                v_load.wait()
            with phase("prep_v"):
                prepare(v_raw, v_hi, v_lo)
        with phase(f"coef{it}"):
            wide = dot(both, v_hi[...], NT)
            coef = wide[:nv] + wide[nv:] + dot(first, v_lo[...], NT)
        if it == 0:
            with phase("wait_barrier"):
                pl.semaphore_wait(barrier, size_all - 1)
        with phase(f"send_partials{it}"):
            send_partials(it, coef)
        meanwhile()
        if it == 0:
            with phase("fillA"):
                fill_near(both, first, 0, leaf_len * 3 // 4)
            send_nodes(it)
            with phase("fillB"):
                fill_near(both, first, leaf_len * 3 // 4, leaf_len)
            u_load.wait()
            with phase("prep_u"):
                prepare(u_raw, u_hi, u_lo)
        else:
            with phase(f"nearA{it}"):
                near_columns(both, first, 0, leaf_len // 2)
            send_nodes(it)
            with phase(f"nearB{it}"):
                near_columns(both, first, leaf_len // 2, leaf_len)
        coef_hi, coef_lo = split2(siblings(it))
        with phase(f"far{it}"):
            wide = dot(jnp.concatenate([coef_hi, coef_lo], axis=0), u_hi[...])
            far = wide[:nv] + wide[nv:] + dot(coef_hi, u_lo[...])
        return live * (image_ref[...] + far) - vector

    def lane_sum(value):
        return jnp.sum(value, axis=1, keepdims=True)

    shift = 1.0 + noise_ref[0]
    gram = {}
    columns = []
    images = []
    beta = None
    raw = basis_ref[0]
    image = operate(0, raw, prepare_points)
    for it in range(ITERS):
        last = it + 1 == ITERS
        def exchange_sums(it=it, raw=raw, image=image, last=last):
            with phase(f"sums{it}"):
                values = [lane_sum(basis_ref[row] * image) for row in range(it)] + [lane_sum(raw * image)]
                values += [lane_sum(basis_ref[row] * raw) for row in range(it)] + [lane_sum(raw * raw)]
                if last:
                    values.append(lane_sum(image * image))
                send_sums(it, values)

        if last:
            exchange_sums()
        else:
            ahead = operate(it + 1, image, exchange_sums)
        sums = read_sums(it, 2 * it + 2 + last)
        with phase(f"ortho{it}"):
            length = jnp.sqrt(sums[2 * it + 1] + epsilon)
            inverse = 1.0 / length
            if it == 0:
                beta = length
            else:
                columns[-1].append(length)
            products = [value * inverse for value in sums[: it + 1]]
            products[it] = products[it] * inverse
            lengths = [value * inverse for value in sums[it + 1 : 2 * it + 2]]
            lengths[it] = lengths[it] * inverse
            vector = raw * inverse
            basis_ref[it] = vector
            for row in range(it + 1):
                gram[row, it] = gram[it, row] = lengths[row]
            column = [products[row] + shift * lengths[row] for row in range(it + 1)]
            moved = [column[row] - shift if row == it else column[row] for row in range(it + 1)]
            columns.append(list(column))
            if last:
                rest = sums[-1] * inverse * inverse
                for row in range(it + 1):
                    inside = -2.0 * products[row]
                    for other in range(it + 1):
                        inside = inside + moved[other] * gram[row, other]
                    rest = rest + moved[row] * inside
                columns[-1].append(jnp.sqrt(jnp.maximum(rest, 0.0) + epsilon))
            else:
                images.append(image * inverse)
                raw = images[it]
                image = ahead * inverse
                for row in range(it + 1):
                    raw = raw - moved[row] * basis_ref[row]
                    image = image - moved[row] * images[row]
    with phase("solve"):
        weights = least_squares(columns, beta)
        solved = weights[0] * basis_ref[0]
        for it in range(1, ITERS):
            solved = solved + weights[it] * basis_ref[it]
    with phase("scatter"):
        parts = jnp.concatenate(split3(solved), axis=0)
        stacked = jnp.concatenate(
            [parts * jnp.where(outer == g, 1.0, 0.0).astype(bf16) for g in range(groups)], axis=0
        )
        got = dot(stacked, pick_ref[...], NT)
        for g in range(groups):
            base = g * 3 * nv
            out_ref[:, g * width : (g + 1) * width] = (
                got[base : base + nv] + got[base + nv : base + 2 * nv] + got[base + 2 * nv : base + 3 * nv]
            )
    for it in range(ITERS):
        landed(others(recv_high, it), part_s.at[it, 1])
        landed(others(recv_low, it), part_s.at[it, 0])
        landed(others(recv_node, it), node_s.at[it])
        landed(others(recv_dots, it), dots_s.at[it])


def per_device(
    size_gx, size_gy,
    coordinates, rhs, leaf_order, leaf_sizes, inverse_scales, noise_var, u_factors, v_factors,
):
    num_vectors, leaf_len = rhs.shape
    num_levels, num_rank = u_factors.shape[0], u_factors.shape[1]
    levels_high = size_gx.bit_length() - 1
    half, lanes = num_vectors // 2, 2 * num_rank
    padded = (num_levels + 1) // 2 * 2 * num_rank
    tile = (half, lanes)
    vmem = pl.BlockSpec(memory_space=pltpu.VMEM)
    smem = pl.BlockSpec(memory_space=pltpu.SMEM)
    any_space = pl.BlockSpec(memory_space=pl.ANY)
    dma = pltpu.SemaphoreType.DMA
    return pl.pallas_call(
        functools.partial(fused, size_gx, size_gy),
        out_shape=jax.ShapeDtypeStruct(rhs.shape, f32),
        in_specs=[vmem, vmem, vmem, smem, smem, smem, any_space, any_space],
        out_specs=vmem,
        scratch_shapes=[
            pltpu.VMEM((leaf_len, leaf_len), bf16),
            pltpu.VMEM((leaf_len, leaf_len), bf16),
            pltpu.VMEM((256, leaf_len), bf16),
            pltpu.VMEM((leaf_len, 128), bf16),
            pltpu.VMEM((128, leaf_len), bf16),
            pltpu.VMEM(u_factors.shape, f32),
            pltpu.VMEM(v_factors.shape, f32),
            pltpu.VMEM((padded, leaf_len), bf16),
            pltpu.VMEM((padded, leaf_len), bf16),
            pltpu.VMEM((padded, leaf_len), bf16),
            pltpu.VMEM((padded, leaf_len), bf16),
            pltpu.VMEM((ITERS,) + rhs.shape, f32),
            pltpu.VMEM(rhs.shape, f32),
            pltpu.VMEM((ITERS, num_levels) + tile, f32),
            pltpu.VMEM((ITERS, size_gy) + tile, f32),
            pltpu.VMEM((ITERS, size_gy, levels_high) + tile, f32),
            pltpu.VMEM((ITERS, levels_high) + tile, f32),
            pltpu.VMEM((ITERS, size_gx) + tile, f32),
            pltpu.VMEM((ITERS, 1, lanes), f32),
            pltpu.VMEM((ITERS, size_gx * size_gy, 1, lanes), f32),
            dma((2,)),
            dma((ITERS, 2)),
            dma((ITERS, 2)),
            dma((ITERS,)),
            dma((ITERS,)),
            dma((ITERS,)),
            dma((ITERS,)),
        ],
        compiler_params=pltpu.CompilerParams(collective_id=0, has_side_effects=True),
        name="gmres",
    )(coordinates, rhs, leaf_order, leaf_sizes, inverse_scales, noise_var, u_factors, v_factors)


def solution(mesh):
    in_specs = (
        P(None, ("gx", "gy")),
        P(None, ("gx", "gy")),
        P(("gx", "gy"), None),
        P(("gx", "gy")),
        P(),
        P(),
        P(None, None, ("gx", "gy")),
        P(None, None, ("gx", "gy")),
    )
    out_specs = P(None, ("gx", "gy"))
    return jax.shard_map(
        functools.partial(per_device, mesh.shape["gx"], mesh.shape["gy"]),
        mesh=mesh, in_specs=in_specs, out_specs=out_specs, check_vma=False,
    )
```

```python
import contextlib
import functools
import math

import jax
import jax.numpy as jnp
from jax import lax
from jax.experimental import pallas as pl
from jax.experimental.pallas import tpu as pltpu
from jax.sharding import PartitionSpec as P

ITERS = 3

epsilon = 1e-06
sqrt_three = math.sqrt(3.0)
log2_e = math.log2(math.e)
MESH = pl.DeviceIdType.MESH
f32 = jnp.float32
bf16 = jnp.bfloat16
NN = (((1,), (0,)), ((), ()))
NT = (((1,), (1,)), ((), ()))


def least_squares(columns, beta):
    count_cols = len(columns)
    cosines = []
    sines = []
    target = [beta] + [jnp.zeros_like(beta)] * count_cols
    upper = []
    for column_idx in range(count_cols):
        entries = list(columns[column_idx])
        for row_idx in range(column_idx):
            first_val = entries[row_idx]
            second_val = entries[row_idx + 1]
            entries[row_idx] = cosines[row_idx] * first_val + sines[row_idx] * second_val
            entries[row_idx + 1] = -sines[row_idx] * first_val + cosines[row_idx] * second_val
        first_val = entries[column_idx]
        second_val = entries[column_idx + 1]
        radius = jnp.sqrt(first_val * first_val + second_val * second_val)
        cosines.append(first_val / radius)
        sines.append(second_val / radius)
        entries[column_idx] = radius
        carried = target[column_idx]
        target[column_idx] = cosines[column_idx] * carried
        target[column_idx + 1] = -sines[column_idx] * carried
        upper.append(entries[: column_idx + 1])
    weights = [None] * count_cols
    for column_idx in reversed(range(count_cols)):
        accum = target[column_idx]
        for later_idx in range(column_idx + 1, count_cols):
            accum = accum - upper[later_idx][column_idx] * weights[later_idx]
        weights[column_idx] = accum / upper[column_idx][column_idx]
    return weights


def flipped(index, bits):
    result = index
    place = 1
    while place <= bits:
        if bits & place:
            result = result + place * (1 - 2 * lax.rem(lax.div(index, place), 2))
        place *= 2
    return result


def split2(value):
    high = value.astype(bf16)
    low = (value - high.astype(f32)).astype(bf16)
    return high, low


def split3(value):
    high = value.astype(bf16)
    rest = value - high.astype(f32)
    mid = rest.astype(bf16)
    low = (rest - mid.astype(f32)).astype(bf16)
    return high, mid, low


@contextlib.contextmanager
def phase(name):
    pl.delay(1)
    with jax.named_scope(name):
        yield
    pl.delay(1)


def dot(left, right, dims=NN):
    return lax.dot_general(left, right, dims, preferred_element_type=f32)


def fused(
    size_gx, size_gy,
    coords_hbm, rhs_hbm, order_hbm, sizes_hbm, inv_hbm, noise_hbm, u_hbm, v_hbm,
    out_ref,
    coords_ref, rhs_ref, order_ref, sizes_ref, inv_ref, noise_ref,
    near_hi, near_lo, pick_ref, left_ref, right_ref, u_raw, v_raw, u_all, v_all, vt_all, mix_all,
    basis_ref, image_ref,
    send_part, recv_low, recv_high, send_node, recv_node,
    send_dots, recv_dots,
    load_sem,
    part_s, part_r, node_s, node_r, dots_s, dots_r,
):
    me_x = lax.axis_index("gx")
    me_y = lax.axis_index("gy")
    levels_low = size_gy.bit_length() - 1
    levels_high = size_gx.bit_length() - 1
    nv, leaf_len = rhs_ref.shape
    num_dims = coords_ref.shape[0]
    num_levels, num_rank = u_raw.shape[0], u_raw.shape[1]
    half = nv // 2
    lanes = 2 * num_rank
    size_all = size_gx * size_gy

    loads = [
        pltpu.make_async_copy(src, dst, load_sem.at[idx])
        for idx, (src, dst) in enumerate((
            (order_hbm, order_ref), (rhs_hbm, rhs_ref), (sizes_hbm, sizes_ref), (v_hbm, v_raw),
            (coords_hbm, coords_ref), (inv_hbm, inv_ref), (noise_hbm, noise_ref), (u_hbm, u_raw),
        ))
    ]
    for load in loads:
        load.start()
    v_load, u_load = loads[3], loads[7]

    peers = [
        (flipped(me_x, apart // size_gy), flipped(me_y, apart % size_gy)) for apart in range(size_all)
    ]
    barrier = pltpu.get_barrier_semaphore()
    for apart in range(1, size_all):
        pl.semaphore_signal(barrier, inc=1, device_id=peers[apart], device_id_type=MESH)

    def send(src, dst, sems, semr, device):
        copy = pltpu.make_async_remote_copy(
            src_ref=src, dst_ref=dst, send_sem=sems, recv_sem=semr,
            device_id=device, device_id_type=MESH,
        )
        copy.start()

    def landed(block, sem):
        pltpu.make_async_copy(block, block, sem).wait()

    for load in loads[:3]:
        load.wait()
    live = jnp.where(
        lax.broadcasted_iota(jnp.int32, (1, leaf_len), 1) < sizes_ref[0], 1.0, 0.0
    ).astype(f32)

    width = 256
    groups = leaf_len // width
    order = order_ref[...]
    outer = lax.div(order, width)
    inner = order - outer * width
    with phase("onehot"):
        pick_ref[...] = jnp.where(
            lax.broadcasted_iota(jnp.int32, (width, leaf_len), 0) == inner, 1.0, 0.0
        ).astype(bf16)
    def gather(stack, pieces):
        rows = stack.shape[0] // pieces
        stacked = jnp.concatenate([stack[:, g * width : (g + 1) * width] for g in range(groups)], axis=0)
        blocks = []
        for start_col in range(0, leaf_len, width):
            cols = slice(start_col, start_col + width)
            got = dot(stacked, pick_ref[:, cols])
            total = jnp.zeros((rows, width), f32)
            for g in range(groups):
                term = None
                for piece in range(pieces):
                    base = (g * pieces + piece) * rows
                    term = got[base : base + rows] if term is None else term + got[base : base + rows]
                total = jnp.where(outer[:, cols] == g, term, total)
            blocks.append(total)
        return jnp.concatenate(blocks, axis=1)

    with phase("gather_rhs"):
        basis_ref[0] = live * gather(jnp.concatenate(split2(rhs_ref[...]), axis=0), 2)

    padded = v_all.shape[0] // 2
    used = num_levels * num_rank

    def prepare(raw, both, mask=None):
        for level in range(num_levels):
            first, second = split2(raw[level] if mask is None else raw[level] * mask)
            low = level * num_rank
            both[low : low + num_rank, :] = first
            both[padded + low : padded + low + num_rank, :] = second
        if padded > used:
            both[used:padded, :] = jnp.zeros((padded - used, leaf_len), bf16)
            both[padded + used :, :] = jnp.zeros((padded - used, leaf_len), bf16)

    lane = lax.broadcasted_iota(jnp.int32, (half, lanes), 1)
    left_side = lane < num_rank

    def swap(value):
        return pltpu.roll(value, num_rank, 1)

    def send_partials(it, coef):
        for level in range(num_levels):
            block = coef[:, (level // 2) * lanes : (level // 2 + 1) * lanes]
            top, bottom = block[:half], block[half:]
            if level % 2 == 0:
                tile = jnp.where(left_side, top, swap(bottom))
            else:
                tile = jnp.where(left_side, swap(top), bottom)
            send_part[it, level] = tile
        for apart in range(1, size_gy):
            send(
                send_part.at[it, pl.ds(levels_low, levels_high)], recv_high.at[it, apart],
                part_s.at[it, 1], part_r.at[it, 1], peers[apart],
            )
        for apart in range(1, size_gy):
            send(
                send_part.at[it, apart.bit_length() - 1], recv_low.at[it, apart],
                part_s.at[it, 0], part_r.at[it, 0], peers[apart],
            )

    def others(ref, it):
        return ref.at[it, pl.ds(1, ref.shape[1] - 1)]

    def send_nodes(it):
        with phase(f"wait_parts{it}"):
            landed(others(recv_high, it), part_r.at[it, 1])
        total = send_part[it, levels_low:num_levels]
        for apart in range(1, size_gy):
            total = total + recv_high[it, apart]
        send_node[it] = total
        for apart in range(1, size_gx):
            send(
                send_node.at[it, apart.bit_length() - 1], recv_node.at[it, apart],
                node_s.at[it], node_r.at[it], peers[apart * size_gy],
            )

    def siblings(it):
        with phase(f"wait_nodes{it}"):
            landed(others(recv_low, it), part_r.at[it, 0])
            landed(others(recv_node, it), node_r.at[it])
        tiles = []
        for count, source in ((levels_low, recv_low), (levels_high, recv_node)):
            for level in range(count):
                total = source[it, 2**level]
                for apart in range(2**level + 1, 2 ** (level + 1)):
                    total = total + source[it, apart]
                tiles.append(total)
        if len(tiles) % 2:
            tiles.append(jnp.zeros_like(tiles[0]))
        blocks = []
        for pair in range(len(tiles) // 2):
            even, odd = tiles[2 * pair], tiles[2 * pair + 1]
            top = jnp.where(left_side, even, swap(odd))
            bottom = jnp.where(left_side, swap(even), odd)
            blocks.append(jnp.concatenate([top, bottom], axis=0))
        return jnp.concatenate(blocks, axis=1)

    slots = lanes // nv
    row16 = lax.broadcasted_iota(jnp.int32, (nv, lanes), 0)
    slot16 = lax.broadcasted_iota(jnp.int32, (nv, lanes), 1) - row16 * slots

    def send_sums(it, values):
        block = jnp.zeros((nv, lanes), f32)
        for idx, value in enumerate(values):
            block = jnp.where(slot16 == idx, value, block)
        send_dots[it] = jnp.sum(block, axis=0, keepdims=True)
        for apart in range(1, size_all):
            send(
                send_dots.at[it], recv_dots.at[it, apart],
                dots_s.at[it], dots_r.at[it], peers[apart],
            )

    def read_sums(it, count):
        with phase(f"wait_sums{it}"):
            landed(others(recv_dots, it), dots_r.at[it])
        terms = [send_dots[it]] + [recv_dots[it, apart] for apart in range(1, size_all)]
        while len(terms) > 1:
            terms = [terms[i] + terms[i + 1] for i in range(0, len(terms), 2)]
        return [
            jnp.sum(jnp.where(slot16 == idx, terms[0], 0.0), axis=1, keepdims=True)
            for idx in range(count)
        ]

    chunk = min(256, leaf_len)

    def doubled(value):
        first, second = split2(value)
        return jnp.concatenate([first, second], axis=0), first

    def product(both, first, hi, lo, dims=NN):
        wide = dot(both, hi, dims)
        return wide[:nv] + wide[nv:] + dot(first, lo, dims)

    def near_columns(both, first, begin, end):
        for low in range(begin, end, chunk):
            high = low + chunk
            cols = slice(low, high)
            total = product(both[:, :high], first[:, :high], near_hi[:high, cols], near_lo[:high, cols])
            if high < leaf_len:
                total = total + product(
                    both[:, high:], first[:, high:], near_hi[cols, high:], near_lo[cols, high:], NT
                )
            image_ref[:, cols] = total

    strip = min(128, chunk)

    def fill_tile(low, base):
        cols = slice(low, low + chunk)
        for start in range(base, base + chunk, strip):
            rows = slice(start, start + strip)
            square = jnp.maximum(dot(left_ref[rows, :], right_ref[:, cols]), 1e-30)
            distance = square * lax.rsqrt(square)
            value = (1.0 + distance) * jnp.exp2(distance * (-log2_e))
            hi, lo = split2(value)
            near_hi[rows, cols] = hi
            near_lo[rows, cols] = lo

    def near_tile(both, first, low, base):
        cols, rows = slice(low, low + chunk), slice(base, base + chunk)
        part = product(both[:, rows], first[:, rows], near_hi[rows, cols], near_lo[rows, cols])
        if base:
            image_ref[:, cols] += part
        else:
            image_ref[:, cols] = part
        if base < low:
            image_ref[:, rows] += product(
                both[:, cols], first[:, cols], near_hi[rows, cols], near_lo[rows, cols], NT
            )

    tiles_all = [(low, base) for low in range(0, leaf_len, chunk) for base in range(0, low + chunk, chunk)]

    def fill_near(both, first, begin, end):
        for idx in range(begin, end):
            low, base = tiles_all[idx]
            fill_tile(low, base)
            if base == low:
                cols = slice(low, low + chunk)
                vt_all[cols, :] = v_all[:, cols].T
            if idx > begin:
                near_tile(both, first, *tiles_all[idx - 1])
        near_tile(both, first, *tiles_all[end - 1])

    def prepare_points():
        for load in loads[4:7]:
            load.wait()
        with phase("gather_pos"):
            coords = jnp.concatenate([coords_ref[...], jnp.zeros((16 - num_dims, leaf_len), f32)], axis=0)
            gathered = gather(jnp.concatenate(split3(coords), axis=0), 3)[:8]
        row8 = lax.broadcasted_iota(jnp.int32, (8, 1), 0)
        with phase("place"):
            scale = jnp.zeros((8, 1), f32)
            for dim in range(num_dims):
                scale = jnp.where(row8 == dim, inv_ref[dim] * sqrt_three, scale)
            place = (gathered - 0.5) * scale
            coarse = jnp.round(place * 4.0) * 0.25
            fine_hi, fine_lo = split2(place - coarse)
            fine_hi, fine_lo = fine_hi.astype(f32), fine_lo.astype(f32)
            fine = fine_hi + fine_lo
            whole_norm = jnp.sum(coarse * coarse, axis=0, keepdims=True)
            rest_norm = jnp.sum(fine * (2.0 * coarse + fine), axis=0, keepdims=True)
        def rows_of(values):
            block = jnp.zeros((8, leaf_len), f32)
            for idx, value in enumerate(values):
                block = jnp.where(row8 == idx, value, block)
            return block

        with phase("lr"):
            norms = [part.astype(f32) for part in split2(whole_norm)]
            rests = [part.astype(f32) for part in split3(rest_norm)]
            ones = [1.0] * 3
            pairs = [
                (-2.0 * coarse, coarse),
                (rows_of(norms + ones[:2]), rows_of(ones[:2] + norms)),
                (rows_of(rests + ones), rows_of(ones + rests)),
                (-2.0 * coarse, fine_hi),
                (-2.0 * coarse, fine_lo),
                (fine_hi, -2.0 * coarse),
                (fine_lo, -2.0 * coarse),
                (fine_hi, -2.0 * fine_hi),
                (fine_hi, -2.0 * fine_lo),
                (fine_lo, -2.0 * fine_hi),
            ]
            blank = jnp.zeros((128 - 8 * len(pairs), leaf_len), f32)
            left_ref[...] = jnp.concatenate([pair[0] for pair in pairs] + [blank], axis=0).T.astype(bf16)
            right_ref[...] = jnp.concatenate([pair[1] for pair in pairs] + [blank], axis=0).astype(bf16)

    def against(both, factors, dims=NN):
        size = factors.shape[0 if dims == NT else 1] // 2
        wide = dot(both, factors[...], dims)
        return wide[:nv, :size] + wide[nv:, :size] + wide[:nv, size:]

    def coefs_of(name, value):
        with phase(f"coefs_{name}"):
            return against(doubled(value)[0], vt_all)

    def far_of(it, coef):
        with phase(f"far{it}"):
            first, second = split2(coef)
            left = jnp.concatenate(
                [
                    jnp.concatenate([first, first], axis=1),
                    jnp.concatenate([second, jnp.zeros_like(second)], axis=1),
                ],
                axis=0,
            )
            wide = dot(left, u_all[...])
            return wide[:nv] + wide[nv:]

    def start_exchange(it, coef):
        with phase(f"send_partials{it}"):
            send_partials(it, coef)

    def operate_first(vector):
        both, first = doubled(vector)
        with phase("wait_v"):
            v_load.wait()
        with phase("prep_v"):
            prepare(v_raw, v_all)
        with phase("coef0"):
            coef = against(both, v_all, NT)
        with phase("wait_barrier"):
            pl.semaphore_wait(barrier, size_all - 1)
        start_exchange(0, coef)
        prepare_points()
        with phase("fillA"):
            fill_near(both, first, 0, len(tiles_all) * 5 // 9)
        send_nodes(0)
        with phase("fillB"):
            fill_near(both, first, len(tiles_all) * 5 // 9, len(tiles_all))
        u_load.wait()
        with phase("prep_u"):
            prepare(u_raw, u_all, live)
        return live * image_ref[...] - vector + far_of(0, siblings(0))

    def operate_near(it, vector, relay):
        both, first = doubled(vector)
        with phase(f"nearA{it}"):
            near_columns(both, first, 0, relay)
        send_nodes(it)
        with phase(f"nearB{it}"):
            near_columns(both, first, relay, leaf_len)
        return live * image_ref[...] - vector

    def prepare_mix():
        with phase("mix"):
            wide = dot(u_all[:used, :], vt_all[...])
            mix = wide[:, :padded] + wide[:, padded:] + dot(u_all[padded : padded + used, :], vt_all[:, :padded])
            first, second = split2(mix)
            mix_all[:used, :padded] = first
            mix_all[:used, padded:] = second
            if padded > used:
                mix_all[used:, :] = jnp.zeros((padded - used, 2 * padded), bf16)

    def lane_sum(value):
        return jnp.sum(value, axis=1, keepdims=True)

    gram = {}
    columns = []
    images = []
    beta = None
    raw = basis_ref[0]
    image = operate_first(raw)
    shift = 1.0 + noise_ref[0]
    coef = coefs_of("first", image)
    coefs = []
    start_exchange(1, coef)
    for it in range(ITERS):
        last = it + 1 == ITERS
        ahead = it + 2 < ITERS
        with phase(f"sums{it}"):
            values = [lane_sum(basis_ref[row] * image) for row in range(it)] + [lane_sum(raw * image)]
            values += [lane_sum(basis_ref[row] * raw) for row in range(it)] + [lane_sum(raw * raw)]
            if last:
                values.append(lane_sum(image * image))
            send_sums(it, values)
        if not last:
            near = operate_near(it + 1, image, leaf_len * (7 if it == 0 else 6) // 8)
            if ahead:
                near_coef = coefs_of(f"near{it}", near)
                if it == 0:
                    prepare_mix()
            found = siblings(it + 1)
        sums = read_sums(it, len(values))
        with phase(f"scalars{it}"):
            length = jnp.sqrt(sums[2 * it + 1] + epsilon)
            inverse = 1.0 / length
            if it == 0:
                beta = length
            else:
                columns[-1].append(length)
            products = [value * inverse for value in sums[: it + 1]]
            products[it] = products[it] * inverse
            lengths = [value * inverse for value in sums[it + 1 : 2 * it + 2]]
            lengths[it] = lengths[it] * inverse
            for row in range(it + 1):
                gram[row, it] = gram[it, row] = lengths[row]
            column = [products[row] + shift * lengths[row] for row in range(it + 1)]
            moved = [column[row] - shift if row == it else column[row] for row in range(it + 1)]
            columns.append(list(column))
        if ahead:
            with phase(f"coefs_next{it}"):
                coefs.append(coef * inverse)
                coef = (near_coef + against(doubled(found)[0], mix_all)) * inverse
                for row in range(it + 1):
                    coef = coef - moved[row] * coefs[row]
            start_exchange(it + 2, coef)
        if not last:
            following = near + far_of(it + 1, found)
        with phase(f"ortho{it}"):
            vector = raw * inverse
            basis_ref[it] = vector
            if last:
                rest = sums[-1] * inverse * inverse
                for row in range(it + 1):
                    inside = -2.0 * products[row]
                    for other in range(it + 1):
                        inside = inside + moved[other] * gram[row, other]
                    rest = rest + moved[row] * inside
                columns[-1].append(jnp.sqrt(jnp.maximum(rest, 0.0) + epsilon))
            else:
                images.append(image * inverse)
                raw = images[it]
                image = following * inverse
                for row in range(it + 1):
                    raw = raw - moved[row] * basis_ref[row]
                    image = image - moved[row] * images[row]
    with phase("solve"):
        weights = least_squares(columns, beta)
        solved = weights[0] * basis_ref[0]
        for it in range(1, ITERS):
            solved = solved + weights[it] * basis_ref[it]
    with phase("scatter"):
        parts = jnp.concatenate(split2(solved), axis=0)
        stacked = jnp.concatenate(
            [parts * jnp.where(outer == g, 1.0, 0.0).astype(bf16) for g in range(groups)], axis=0
        )
        got = dot(stacked, pick_ref[...], NT)
        for g in range(groups):
            base = 2 * g * nv
            out_ref[:, g * width : (g + 1) * width] = got[base : base + nv] + got[base + nv : base + 2 * nv]
    for it in range(ITERS):
        landed(others(recv_high, it), part_s.at[it, 1])
        landed(others(recv_low, it), part_s.at[it, 0])
        landed(others(recv_node, it), node_s.at[it])
        landed(others(recv_dots, it), dots_s.at[it])


def per_device(
    size_gx, size_gy,
    coordinates, rhs, leaf_order, leaf_sizes, inverse_scales, noise_var, u_factors, v_factors,
):
    num_vectors, leaf_len = rhs.shape
    num_levels, num_rank = u_factors.shape[0], u_factors.shape[1]
    levels_high = size_gx.bit_length() - 1
    half, lanes = num_vectors // 2, 2 * num_rank
    padded = (num_levels + 1) // 2 * 2 * num_rank
    tile = (half, lanes)
    vmem = pl.BlockSpec(memory_space=pltpu.VMEM)
    hbm = pl.BlockSpec(memory_space=pltpu.HBM)
    dma = pltpu.SemaphoreType.DMA
    return pl.pallas_call(
        functools.partial(fused, size_gx, size_gy),
        out_shape=jax.ShapeDtypeStruct(rhs.shape, f32),
        in_specs=[hbm] * 8,
        out_specs=vmem,
        scratch_shapes=[
            pltpu.VMEM(coordinates.shape, f32),
            pltpu.VMEM(rhs.shape, f32),
            pltpu.VMEM(leaf_order.shape, jnp.int32),
            pltpu.SMEM(leaf_sizes.shape, jnp.int32),
            pltpu.SMEM(inverse_scales.shape, f32),
            pltpu.SMEM(noise_var.shape, f32),
            pltpu.VMEM((leaf_len, leaf_len), bf16),
            pltpu.VMEM((leaf_len, leaf_len), bf16),
            pltpu.VMEM((256, leaf_len), bf16),
            pltpu.VMEM((leaf_len, 128), bf16),
            pltpu.VMEM((128, leaf_len), bf16),
            pltpu.VMEM(u_factors.shape, f32),
            pltpu.VMEM(v_factors.shape, f32),
            pltpu.VMEM((2 * padded, leaf_len), bf16),
            pltpu.VMEM((2 * padded, leaf_len), bf16),
            pltpu.VMEM((leaf_len, 2 * padded), bf16),
            pltpu.VMEM((padded, 2 * padded), bf16),
            pltpu.VMEM((ITERS,) + rhs.shape, f32),
            pltpu.VMEM(rhs.shape, f32),
            pltpu.VMEM((ITERS, num_levels) + tile, f32),
            pltpu.VMEM((ITERS, size_gy) + tile, f32),
            pltpu.VMEM((ITERS, size_gy, levels_high) + tile, f32),
            pltpu.VMEM((ITERS, levels_high) + tile, f32),
            pltpu.VMEM((ITERS, size_gx) + tile, f32),
            pltpu.VMEM((ITERS, 1, lanes), f32),
            pltpu.VMEM((ITERS, size_gx * size_gy, 1, lanes), f32),
            dma((8,)),
            dma((ITERS, 2)),
            dma((ITERS, 2)),
            dma((ITERS,)),
            dma((ITERS,)),
            dma((ITERS,)),
            dma((ITERS,)),
        ],
        compiler_params=pltpu.CompilerParams(collective_id=0, has_side_effects=True),
        name="gmres",
    )(coordinates, rhs, leaf_order, leaf_sizes, inverse_scales, noise_var, u_factors, v_factors)


def solution(mesh):
    in_specs = (
        P(None, ("gx", "gy")),
        P(None, ("gx", "gy")),
        P(("gx", "gy"), None),
        P(("gx", "gy")),
        P(),
        P(),
        P(None, None, ("gx", "gy")),
        P(None, None, ("gx", "gy")),
    )
    out_specs = P(None, ("gx", "gy"))
    return jax.shard_map(
        functools.partial(per_device, mesh.shape["gx"], mesh.shape["gy"]),
        mesh=mesh, in_specs=in_specs, out_specs=out_specs, check_vma=False,
    )
```

```python
import contextlib
import functools
import math

import jax
import jax.numpy as jnp
from jax import lax
from jax.experimental import pallas as pl
from jax.experimental.pallas import tpu as pltpu
from jax.sharding import PartitionSpec as P

ITERS = 3

epsilon = 1e-06
sqrt_three = math.sqrt(3.0)
log2_e = math.log2(math.e)
MESH = pl.DeviceIdType.MESH
f32 = jnp.float32
bf16 = jnp.bfloat16
NN = (((1,), (0,)), ((), ()))
NT = (((1,), (1,)), ((), ()))


def least_squares(columns, beta):
    count_cols = len(columns)
    cosines = []
    sines = []
    target = [beta] + [jnp.zeros_like(beta)] * count_cols
    upper = []
    for column_idx in range(count_cols):
        entries = list(columns[column_idx])
        for row_idx in range(column_idx):
            first_val = entries[row_idx]
            second_val = entries[row_idx + 1]
            entries[row_idx] = cosines[row_idx] * first_val + sines[row_idx] * second_val
            entries[row_idx + 1] = -sines[row_idx] * first_val + cosines[row_idx] * second_val
        first_val = entries[column_idx]
        second_val = entries[column_idx + 1]
        radius = jnp.sqrt(first_val * first_val + second_val * second_val)
        cosines.append(first_val / radius)
        sines.append(second_val / radius)
        entries[column_idx] = radius
        carried = target[column_idx]
        target[column_idx] = cosines[column_idx] * carried
        target[column_idx + 1] = -sines[column_idx] * carried
        upper.append(entries[: column_idx + 1])
    weights = [None] * count_cols
    for column_idx in reversed(range(count_cols)):
        accum = target[column_idx]
        for later_idx in range(column_idx + 1, count_cols):
            accum = accum - upper[later_idx][column_idx] * weights[later_idx]
        weights[column_idx] = accum / upper[column_idx][column_idx]
    return weights


def flipped(index, bits):
    result = index
    place = 1
    while place <= bits:
        if bits & place:
            result = result + place * (1 - 2 * lax.rem(lax.div(index, place), 2))
        place *= 2
    return result


def split2(value):
    high = value.astype(bf16)
    low = (value - high.astype(f32)).astype(bf16)
    return high, low


def split3(value):
    high = value.astype(bf16)
    rest = value - high.astype(f32)
    mid = rest.astype(bf16)
    low = (rest - mid.astype(f32)).astype(bf16)
    return high, mid, low


@contextlib.contextmanager
def phase(name):
    pl.delay(1)
    with jax.named_scope(name):
        yield
    pl.delay(1)


def dot(left, right, dims=NN):
    return lax.dot_general(left, right, dims, preferred_element_type=f32)


def fused(
    size_gx, size_gy,
    coords_hbm, rhs_hbm, order_hbm, sizes_hbm, inv_hbm, noise_hbm, u_hbm, v_hbm,
    out_ref,
    coords_ref, rhs_ref, order_ref, sizes_ref, inv_ref, noise_ref,
    near_hi, near_lo, pick_ref, left_ref, right_ref, u_raw, v_raw, u_all, v_all, vt_all, mix_all,
    basis_ref, image_ref,
    send_low, send_high, recv_low, recv_high, send_node, recv_node, spread_ref,
    send_dots, recv_dots,
    load_sem,
    part_s, part_r, node_s, node_r, dots_s, dots_r,
):
    me_x = lax.axis_index("gx")
    me_y = lax.axis_index("gy")
    levels_low = size_gy.bit_length() - 1
    levels_high = size_gx.bit_length() - 1
    nv, leaf_len = rhs_ref.shape
    num_dims = coords_ref.shape[0]
    num_levels, num_rank = u_raw.shape[0], u_raw.shape[1]
    half = nv // 2
    quarter = nv // 4
    lanes = 2 * num_rank
    my_core = lax.rem(me_y, 2)
    size_all = size_gx * size_gy

    loads = [
        pltpu.make_async_copy(src, dst, load_sem.at[idx])
        for idx, (src, dst) in enumerate((
            (order_hbm, order_ref), (rhs_hbm, rhs_ref), (sizes_hbm, sizes_ref), (v_hbm, v_raw),
            (coords_hbm, coords_ref), (inv_hbm, inv_ref), (noise_hbm, noise_ref), (u_hbm, u_raw),
        ))
    ]
    for load in loads:
        load.start()
    v_load, u_load = loads[3], loads[7]

    peers = [
        (flipped(me_x, apart // size_gy), flipped(me_y, apart % size_gy)) for apart in range(size_all)
    ]
    barrier = pltpu.get_barrier_semaphore()
    for apart in range(1, size_all):
        pl.semaphore_signal(barrier, inc=1, device_id=peers[apart], device_id_type=MESH)

    def send(src, dst, sems, semr, device):
        copy = pltpu.make_async_remote_copy(
            src_ref=src, dst_ref=dst, send_sem=sems, recv_sem=semr,
            device_id=device, device_id_type=MESH,
        )
        copy.start()

    def landed(block, sem):
        pltpu.make_async_copy(block, block, sem).wait()

    for load in loads[:3]:
        load.wait()
    live = jnp.where(
        lax.broadcasted_iota(jnp.int32, (1, leaf_len), 1) < sizes_ref[0], 1.0, 0.0
    ).astype(f32)

    width = 256
    groups = leaf_len // width
    order = order_ref[...]
    outer = lax.div(order, width)
    inner = order - outer * width
    with phase("onehot"):
        pick_ref[...] = jnp.where(
            lax.broadcasted_iota(jnp.int32, (width, leaf_len), 0) == inner, 1.0, 0.0
        ).astype(bf16)
    def gather(stack, pieces):
        rows = stack.shape[0] // pieces
        stacked = jnp.concatenate([stack[:, g * width : (g + 1) * width] for g in range(groups)], axis=0)
        blocks = []
        for start_col in range(0, leaf_len, width):
            cols = slice(start_col, start_col + width)
            got = dot(stacked, pick_ref[:, cols])
            total = jnp.zeros((rows, width), f32)
            for g in range(groups):
                term = None
                for piece in range(pieces):
                    base = (g * pieces + piece) * rows
                    term = got[base : base + rows] if term is None else term + got[base : base + rows]
                total = jnp.where(outer[:, cols] == g, term, total)
            blocks.append(total)
        return jnp.concatenate(blocks, axis=1)

    with phase("gather_rhs"):
        basis_ref[0] = live * gather(jnp.concatenate(split2(rhs_ref[...]), axis=0), 2)

    padded = v_all.shape[0] // 2
    used = num_levels * num_rank

    def prepare(raw, both, mask=None):
        for level in range(num_levels):
            first, second = split2(raw[level] if mask is None else raw[level] * mask)
            low = level * num_rank
            both[low : low + num_rank, :] = first
            both[padded + low : padded + low + num_rank, :] = second
        if padded > used:
            both[used:padded, :] = jnp.zeros((padded - used, leaf_len), bf16)
            both[padded + used :, :] = jnp.zeros((padded - used, leaf_len), bf16)

    lane = lax.broadcasted_iota(jnp.int32, (half, lanes), 1)
    left_side = lane < num_rank

    def swap(value):
        return pltpu.roll(value, num_rank, 1)

    def send_partials(it, coef):
        for level in range(num_levels):
            block = coef[:, (level // 2) * lanes : (level // 2 + 1) * lanes]
            top, bottom = block[:half], block[half:]
            if level % 2 == 0:
                tile = jnp.where(left_side, top, swap(bottom))
            else:
                tile = jnp.where(left_side, swap(top), bottom)
            if level < levels_low:
                send_low[it, level] = tile
            else:
                for part in range(2):
                    send_high[it, part, level - levels_low] = tile[part * quarter : (part + 1) * quarter]
        for apart in reversed(range(1, size_gy)):
            send(
                send_high.at[it, lax.rem(peers[apart][1], 2)], recv_high.at[it, apart],
                part_s.at[it, 1], part_r.at[it, 1], peers[apart],
            )
        for apart in reversed(range(1, size_gy)):
            send(
                send_low.at[it, apart.bit_length() - 1], recv_low.at[it, apart],
                part_s.at[it, 0], part_r.at[it, 0], peers[apart],
            )

    def others(ref, it):
        return ref.at[it, pl.ds(1, ref.shape[1] - 1)]

    def send_nodes(it):
        with phase(f"wait_parts{it}"):
            landed(others(recv_high, it), part_r.at[it, 1])
        total = send_high[it, my_core]
        for apart in range(1, size_gy):
            total = total + recv_high[it, apart]
        send_node[it] = total
        for apart in reversed(range(1, size_gx)):
            for core in range(2):
                send(
                    send_node.at[it, apart.bit_length() - 1], recv_node.at[it, apart, my_core],
                    node_s.at[it], node_r.at[it], peers[apart * size_gy + core],
                )

    def siblings(it):
        with phase(f"wait_nodes{it}"):
            landed(others(recv_low, it), part_r.at[it, 0])
            landed(others(recv_node, it), node_r.at[it])
        tiles = []
        for count, source in ((levels_low, recv_low), (levels_high, recv_node)):
            for level in range(count):
                total = source[it, 2**level]
                for apart in range(2**level + 1, 2 ** (level + 1)):
                    total = total + source[it, apart]
                if source is recv_node:
                    total = jnp.concatenate([total[0], total[1]], axis=0)
                tiles.append(total)
        if len(tiles) % 2:
            tiles.append(jnp.zeros_like(tiles[0]))
        blocks = []
        for pair in range(len(tiles) // 2):
            even, odd = tiles[2 * pair], tiles[2 * pair + 1]
            top = jnp.where(left_side, even, swap(odd))
            bottom = jnp.where(left_side, swap(even), odd)
            blocks.append(jnp.concatenate([top, bottom], axis=0))
        return jnp.concatenate(blocks, axis=1)

    slots = lanes // nv
    row16 = lax.broadcasted_iota(jnp.int32, (nv, lanes), 0)
    slot16 = lax.broadcasted_iota(jnp.int32, (nv, lanes), 1) - row16 * slots

    def send_sums(it, values):
        block = jnp.zeros((nv, lanes), f32)
        for idx, value in enumerate(values):
            block = jnp.where(slot16 == idx, value, block)
        send_dots[it] = jnp.sum(block, axis=0, keepdims=True)
        for apart in reversed(range(1, size_all)):
            send(
                send_dots.at[it], recv_dots.at[it, apart],
                dots_s.at[it], dots_r.at[it], peers[apart],
            )

    def read_sums(it, count):
        with phase(f"wait_sums{it}"):
            landed(others(recv_dots, it), dots_r.at[it])
        terms = [send_dots[it]] + [recv_dots[it, apart] for apart in range(1, size_all)]
        while len(terms) > 1:
            terms = [terms[i] + terms[i + 1] for i in range(0, len(terms), 2)]
        return [
            jnp.sum(jnp.where(slot16 == idx, terms[0], 0.0), axis=1, keepdims=True)
            for idx in range(count)
        ]

    chunk = min(256, leaf_len)

    def doubled(value):
        first, second = split2(value)
        return jnp.concatenate([first, second], axis=0), first

    def product(both, first, hi, lo, dims=NN):
        wide = dot(both, hi, dims)
        return wide[:nv] + wide[nv:] + dot(first, lo, dims)

    def near_columns(both, first, begin, end):
        for low in range(begin, end, chunk):
            high = low + chunk
            cols = slice(low, high)
            total = product(both[:, :high], first[:, :high], near_hi[:high, cols], near_lo[:high, cols])
            if high < leaf_len:
                total = total + product(
                    both[:, high:], first[:, high:], near_hi[cols, high:], near_lo[cols, high:], NT
                )
            image_ref[:, cols] = total

    strip = min(256, chunk)

    def fill_tile(low, base):
        cols = slice(low, low + chunk)
        for start in range(base, base + chunk, strip):
            rows = slice(start, start + strip)
            square = jnp.maximum(dot(left_ref[rows, :], right_ref[:, cols]), 1e-30)
            distance = square * lax.rsqrt(square)
            value = (1.0 + distance) * jnp.exp2(distance * (-log2_e))
            hi, lo = split2(value)
            near_hi[rows, cols] = hi
            near_lo[rows, cols] = lo

    def near_tile(both, first, low, base):
        cols, rows = slice(low, low + chunk), slice(base, base + chunk)
        part = product(both[:, rows], first[:, rows], near_hi[rows, cols], near_lo[rows, cols])
        if base:
            image_ref[:, cols] += part
        else:
            image_ref[:, cols] = part
        if base < low:
            image_ref[:, rows] += product(
                both[:, cols], first[:, cols], near_hi[rows, cols], near_lo[rows, cols], NT
            )

    tiles_all = [(low, base) for low in range(0, leaf_len, chunk) for base in range(0, low + chunk, chunk)]

    def fill_near(both, first, begin, end):
        for idx in range(begin, end):
            low, base = tiles_all[idx]
            fill_tile(low, base)
            if base == low:
                cols = slice(low, low + chunk)
                vt_all[cols, :] = v_all[:, cols].T
            if idx > begin:
                near_tile(both, first, *tiles_all[idx - 1])
        near_tile(both, first, *tiles_all[end - 1])

    def prepare_points():
        for load in loads[4:7]:
            load.wait()
        with phase("gather_pos"):
            parts = [part.astype(f32) for part in split3(coords_ref[...])]
            spare = jnp.zeros((16 - 3 * num_dims, leaf_len), f32)
            got = gather(jnp.concatenate(parts + [spare], axis=0).astype(bf16), 1)
            gathered = got[:num_dims] + got[num_dims : 2 * num_dims] + got[2 * num_dims : 3 * num_dims]
            gathered = jnp.concatenate([gathered, jnp.zeros((8 - num_dims, leaf_len), f32)], axis=0)
        row8 = lax.broadcasted_iota(jnp.int32, (8, 1), 0)
        with phase("place"):
            scale = jnp.zeros((8, 1), f32)
            for dim in range(num_dims):
                scale = jnp.where(row8 == dim, inv_ref[dim] * sqrt_three, scale)
            place = (gathered - 0.5) * scale
            coarse = jnp.round(place * 4.0) * 0.25
            fine_hi, fine_lo = split2(place - coarse)
            fine_hi, fine_lo = fine_hi.astype(f32), fine_lo.astype(f32)
            fine = fine_hi + fine_lo
            whole_norm = jnp.sum(coarse * coarse, axis=0, keepdims=True)
            rest_norm = jnp.sum(fine * (2.0 * coarse + fine), axis=0, keepdims=True)
        def rows_of(values):
            block = jnp.zeros((8, leaf_len), f32)
            for idx, value in enumerate(values):
                block = jnp.where(row8 == idx, value, block)
            return block

        with phase("lr"):
            norms = [part.astype(f32) for part in split2(whole_norm)]
            rests = [part.astype(f32) for part in split3(rest_norm)]
            ones = [1.0] * 3
            pairs = [
                (-2.0 * coarse, coarse),
                (rows_of(norms + ones[:2]), rows_of(ones[:2] + norms)),
                (rows_of(rests + ones), rows_of(ones + rests)),
                (-2.0 * coarse, fine_hi),
                (-2.0 * coarse, fine_lo),
                (fine_hi, -2.0 * coarse),
                (fine_lo, -2.0 * coarse),
                (fine_hi, -2.0 * fine_hi),
                (fine_hi, -2.0 * fine_lo),
                (fine_lo, -2.0 * fine_hi),
            ]
            blank = jnp.zeros((128 - 8 * len(pairs), leaf_len), f32)
            left_ref[...] = jnp.concatenate([pair[0] for pair in pairs] + [blank], axis=0).T.astype(bf16)
            right_ref[...] = jnp.concatenate([pair[1] for pair in pairs] + [blank], axis=0).astype(bf16)

    def against(both, factors):
        size = factors.shape[1] // 2
        wide = dot(both, factors[...])
        return wide[:nv, :size] + wide[nv:, :size] + wide[:nv, size:]

    def coefs_of(name, value):
        with phase(f"coefs_{name}"):
            return product(*doubled(value), vt_all[:, :padded], vt_all[:, padded:])

    def far_of(it, coef):
        with phase(f"far{it}"):
            first, second = split2(coef)
            left = jnp.concatenate(
                [
                    jnp.concatenate([first, first], axis=1),
                    jnp.concatenate([second, jnp.zeros_like(second)], axis=1),
                ],
                axis=0,
            )
            wide = dot(left, u_all[...])
            return wide[:nv] + wide[nv:]

    def start_exchange(it, coef):
        with phase(f"send_partials{it}"):
            send_partials(it, coef)

    def operate_first(vector):
        both, first = doubled(vector)
        with phase("wait_v"):
            v_load.wait()
        with phase("prep_v"):
            prepare(v_raw, v_all)
        with phase("coef0"):
            coef = product(both, first, v_all[:padded, :], v_all[padded:, :], NT)
        with phase("wait_barrier"):
            pl.semaphore_wait(barrier, size_all - 1)
        start_exchange(0, coef)
        prepare_points()
        with phase("fillA"):
            fill_near(both, first, 0, len(tiles_all) * 5 // 9)
        send_nodes(0)
        with phase("fillB"):
            fill_near(both, first, len(tiles_all) * 5 // 9, len(tiles_all))
        u_load.wait()
        with phase("prep_u"):
            prepare(u_raw, u_all, live)
        return live * image_ref[...] - vector + far_of(0, siblings(0))

    def operate_near(it, vector, relay):
        both, first = doubled(vector)
        with phase(f"nearA{it}"):
            near_columns(both, first, 0, relay)
        send_nodes(it)
        with phase(f"nearB{it}"):
            near_columns(both, first, relay, leaf_len)
        return live * image_ref[...] - vector

    def prepare_mix():
        with phase("mix"):
            wide = dot(u_all[:used, :], vt_all[...])
            mix = wide[:, :padded] + wide[:, padded:] + dot(u_all[padded : padded + used, :], vt_all[:, :padded])
            first, second = split2(mix)
            mix_all[:used, :padded] = first
            mix_all[:used, padded:] = second
            if padded > used:
                mix_all[used:, :] = jnp.zeros((padded - used, 2 * padded), bf16)

    def lane_sum(value):
        return jnp.sum(value, axis=1, keepdims=True)

    gram = {}
    columns = []
    images = []
    beta = None
    def spread(row, vector):
        parts = jnp.concatenate(split2(vector), axis=0)
        stacked = jnp.concatenate(
            [parts * jnp.where(outer == g, 1.0, 0.0).astype(bf16) for g in range(groups)], axis=0
        )
        got = dot(stacked, pick_ref[...], NT)
        for g in range(groups):
            base = 2 * g * nv
            spread_ref[row, :, g * width : (g + 1) * width] = got[base : base + nv] + got[base + nv : base + 2 * nv]

    last_it = ITERS - 1
    raw = basis_ref[0]
    image = operate_first(raw)
    shift = 1.0 + noise_ref[0]
    coef = coefs_of("first", image)
    coefs = []
    start_exchange(1, coef)
    for it in range(ITERS):
        last = it + 1 == ITERS
        ahead = it + 2 < ITERS
        with phase(f"sums{it}"):
            values = [lane_sum(basis_ref[row] * image) for row in range(it)] + [lane_sum(raw * image)]
            values += [lane_sum(basis_ref[row] * raw) for row in range(it)] + [lane_sum(raw * raw)]
            if last:
                values.append(lane_sum(image * image))
            send_sums(it, values)
        if not last:
            near = operate_near(it + 1, image, leaf_len * (6 if it == 0 else 4) // 8)
            if ahead:
                near_coef = coefs_of(f"near{it}", near)
                if it == 0:
                    prepare_mix()
        else:
            for row in range(ITERS):
                with phase(f"spread{row}"):
                    spread(row, raw if row == it else basis_ref[row])
        sums = read_sums(it, len(values))
        with phase(f"scalars{it}"):
            length = jnp.sqrt(sums[2 * it + 1] + epsilon)
            inverse = 1.0 / length
            if it == 0:
                beta = length
            else:
                columns[-1].append(length)
            products = [value * inverse for value in sums[: it + 1]]
            products[it] = products[it] * inverse
            lengths = [value * inverse for value in sums[it + 1 : 2 * it + 2]]
            lengths[it] = lengths[it] * inverse
            for row in range(it + 1):
                gram[row, it] = gram[it, row] = lengths[row]
            column = [products[row] + shift * lengths[row] for row in range(it + 1)]
            moved = [column[row] - shift if row == it else column[row] for row in range(it + 1)]
            columns.append(list(column))
        if not last:
            found = siblings(it + 1)
        if ahead:
            with phase(f"coefs_next{it}"):
                coefs.append(coef * inverse)
                coef = (near_coef + against(doubled(found)[0], mix_all)) * inverse
                for row in range(it + 1):
                    coef = coef - moved[row] * coefs[row]
            start_exchange(it + 2, coef)
        if not last:
            following = near + far_of(it + 1, found)
        with phase(f"ortho{it}"):
            vector = raw * inverse
            basis_ref[it] = vector
            if last:
                rest = sums[-1] * inverse * inverse
                for row in range(it + 1):
                    inside = -2.0 * products[row]
                    for other in range(it + 1):
                        inside = inside + moved[other] * gram[row, other]
                    rest = rest + moved[row] * inside
                columns[-1].append(jnp.sqrt(jnp.maximum(rest, 0.0) + epsilon))
            else:
                images.append(image * inverse)
                raw = images[it]
                image = following * inverse
                for row in range(it + 1):
                    raw = raw - moved[row] * basis_ref[row]
                    image = image - moved[row] * images[row]
    with phase("solve"):
        weights = least_squares(columns, beta)
        weights[last_it] = weights[last_it] * inverse
        solved = weights[0] * spread_ref[0]
        for it in range(1, ITERS):
            solved = solved + weights[it] * spread_ref[it]
        out_ref[...] = solved
    for it in range(ITERS):
        landed(others(recv_high, it), part_s.at[it, 1])
        landed(others(recv_low, it), part_s.at[it, 0])
        landed(others(recv_node, it), node_s.at[it])
        landed(others(recv_dots, it), dots_s.at[it])


def per_device(
    size_gx, size_gy,
    coordinates, rhs, leaf_order, leaf_sizes, inverse_scales, noise_var, u_factors, v_factors,
):
    num_vectors, leaf_len = rhs.shape
    num_levels, num_rank = u_factors.shape[0], u_factors.shape[1]
    levels_high = size_gx.bit_length() - 1
    half, lanes = num_vectors // 2, 2 * num_rank
    padded = (num_levels + 1) // 2 * 2 * num_rank
    tile, part = (half, lanes), (half // 2, lanes)
    levels_low = size_gy.bit_length() - 1
    vmem = pl.BlockSpec(memory_space=pltpu.VMEM)
    hbm = pl.BlockSpec(memory_space=pltpu.HBM)
    dma = pltpu.SemaphoreType.DMA
    return pl.pallas_call(
        functools.partial(fused, size_gx, size_gy),
        out_shape=jax.ShapeDtypeStruct(rhs.shape, f32),
        in_specs=[hbm] * 8,
        out_specs=vmem,
        scratch_shapes=[
            pltpu.VMEM(coordinates.shape, f32),
            pltpu.VMEM(rhs.shape, f32),
            pltpu.VMEM(leaf_order.shape, jnp.int32),
            pltpu.SMEM(leaf_sizes.shape, jnp.int32),
            pltpu.SMEM(inverse_scales.shape, f32),
            pltpu.SMEM(noise_var.shape, f32),
            pltpu.VMEM((leaf_len, leaf_len), bf16),
            pltpu.VMEM((leaf_len, leaf_len), bf16),
            pltpu.VMEM((256, leaf_len), bf16),
            pltpu.VMEM((leaf_len, 128), bf16),
            pltpu.VMEM((128, leaf_len), bf16),
            pltpu.VMEM(u_factors.shape, f32),
            pltpu.VMEM(v_factors.shape, f32),
            pltpu.VMEM((2 * padded, leaf_len), bf16),
            pltpu.VMEM((2 * padded, leaf_len), bf16),
            pltpu.VMEM((leaf_len, 2 * padded), bf16),
            pltpu.VMEM((padded, 2 * padded), bf16),
            pltpu.VMEM((ITERS,) + rhs.shape, f32),
            pltpu.VMEM(rhs.shape, f32),
            pltpu.VMEM((ITERS, levels_low) + tile, f32),
            pltpu.VMEM((ITERS, 2, levels_high) + part, f32),
            pltpu.VMEM((ITERS, size_gy) + tile, f32),
            pltpu.VMEM((ITERS, size_gy, levels_high) + part, f32),
            pltpu.VMEM((ITERS, levels_high) + part, f32),
            pltpu.VMEM((ITERS, size_gx, 2) + part, f32),
            pltpu.VMEM((ITERS,) + rhs.shape, f32),
            pltpu.VMEM((ITERS, 1, lanes), f32),
            pltpu.VMEM((ITERS, size_gx * size_gy, 1, lanes), f32),
            dma((8,)),
            dma((ITERS, 2)),
            dma((ITERS, 2)),
            dma((ITERS,)),
            dma((ITERS,)),
            dma((ITERS,)),
            dma((ITERS,)),
        ],
        compiler_params=pltpu.CompilerParams(collective_id=0, has_side_effects=True),
        name="gmres",
    )(coordinates, rhs, leaf_order, leaf_sizes, inverse_scales, noise_var, u_factors, v_factors)


def solution(mesh):
    in_specs = (
        P(None, ("gx", "gy")),
        P(None, ("gx", "gy")),
        P(("gx", "gy"), None),
        P(("gx", "gy")),
        P(),
        P(),
        P(None, None, ("gx", "gy")),
        P(None, None, ("gx", "gy")),
    )
    out_specs = P(None, ("gx", "gy"))
    return jax.shard_map(
        functools.partial(per_device, mesh.shape["gx"], mesh.shape["gy"]),
        mesh=mesh, in_specs=in_specs, out_specs=out_specs, check_vma=False,
    )
```

```python
import contextlib
import functools
import math

import jax
import jax.numpy as jnp
from jax import lax
from jax.experimental import pallas as pl
from jax.experimental.pallas import tpu as pltpu
from jax.sharding import PartitionSpec as P

ITERS = 3

epsilon = 1e-06
sqrt_three = math.sqrt(3.0)
log2_e = math.log2(math.e)
MESH = pl.DeviceIdType.MESH
f32 = jnp.float32
bf16 = jnp.bfloat16
NN = (((1,), (0,)), ((), ()))
NT = (((1,), (1,)), ((), ()))


def least_squares(columns, beta):
    count_cols = len(columns)
    cosines = []
    sines = []
    target = [beta] + [jnp.zeros_like(beta)] * count_cols
    upper = []
    for column_idx in range(count_cols):
        entries = list(columns[column_idx])
        for row_idx in range(column_idx):
            first_val = entries[row_idx]
            second_val = entries[row_idx + 1]
            entries[row_idx] = cosines[row_idx] * first_val + sines[row_idx] * second_val
            entries[row_idx + 1] = -sines[row_idx] * first_val + cosines[row_idx] * second_val
        first_val = entries[column_idx]
        second_val = entries[column_idx + 1]
        radius = jnp.sqrt(first_val * first_val + second_val * second_val)
        cosines.append(first_val / radius)
        sines.append(second_val / radius)
        entries[column_idx] = radius
        carried = target[column_idx]
        target[column_idx] = cosines[column_idx] * carried
        target[column_idx + 1] = -sines[column_idx] * carried
        upper.append(entries[: column_idx + 1])
    weights = [None] * count_cols
    for column_idx in reversed(range(count_cols)):
        accum = target[column_idx]
        for later_idx in range(column_idx + 1, count_cols):
            accum = accum - upper[later_idx][column_idx] * weights[later_idx]
        weights[column_idx] = accum / upper[column_idx][column_idx]
    return weights


def flipped(index, bits):
    result = index
    place = 1
    while place <= bits:
        if bits & place:
            result = result + place * (1 - 2 * lax.rem(lax.div(index, place), 2))
        place *= 2
    return result


def split2(value):
    high = value.astype(bf16)
    low = (value - high.astype(f32)).astype(bf16)
    return high, low


def split3(value):
    high = value.astype(bf16)
    rest = value - high.astype(f32)
    mid = rest.astype(bf16)
    low = (rest - mid.astype(f32)).astype(bf16)
    return high, mid, low


@contextlib.contextmanager
def phase(name):
    pl.delay(1)
    with jax.named_scope(name):
        yield
    pl.delay(1)


def dot(left, right, dims=NN):
    return lax.dot_general(left, right, dims, preferred_element_type=f32)


def fused(
    size_gx, size_gy,
    coords_hbm, rhs_hbm, order_hbm, sizes_hbm, inv_hbm, noise_hbm, u_hbm, v_hbm,
    out_ref,
    coords_ref, rhs_ref, order_ref, sizes_ref, inv_ref, noise_ref,
    near_hi, near_lo, pick_ref, left_ref, right_ref, u_raw, v_raw, u_all, v_all, vt_all, mix_all,
    basis_ref, image_ref,
    send_low, send_high, recv_low, recv_high, send_node, recv_node, spread_ref,
    send_dots, recv_dots,
    load_sem,
    part_s, part_r, node_s, node_r, dots_s, dots_r,
):
    me_x = lax.axis_index("gx")
    me_y = lax.axis_index("gy")
    levels_low = size_gy.bit_length() - 1
    levels_high = size_gx.bit_length() - 1
    nv, leaf_len = rhs_ref.shape
    num_dims = coords_ref.shape[0]
    num_levels, num_rank = u_raw.shape[0], u_raw.shape[1]
    half = nv // 2
    quarter = nv // 4
    lanes = 2 * num_rank
    my_core = lax.rem(me_y, 2)
    size_all = size_gx * size_gy

    loads = [
        pltpu.make_async_copy(src, dst, load_sem.at[idx])
        for idx, (src, dst) in enumerate((
            (order_hbm, order_ref), (rhs_hbm, rhs_ref), (sizes_hbm, sizes_ref), (v_hbm, v_raw),
            (coords_hbm, coords_ref), (inv_hbm, inv_ref), (noise_hbm, noise_ref), (u_hbm, u_raw),
        ))
    ]
    for load in loads:
        load.start()
    v_load, u_load = loads[3], loads[7]

    peers = [
        (flipped(me_x, apart // size_gy), flipped(me_y, apart % size_gy)) for apart in range(size_all)
    ]
    barrier = pltpu.get_barrier_semaphore()
    for apart in range(1, size_all):
        pl.semaphore_signal(barrier, inc=1, device_id=peers[apart], device_id_type=MESH)

    def send(src, dst, sems, semr, device):
        copy = pltpu.make_async_remote_copy(
            src_ref=src, dst_ref=dst, send_sem=sems, recv_sem=semr,
            device_id=device, device_id_type=MESH,
        )
        copy.start()

    def landed(block, sem):
        pltpu.make_async_copy(block, block, sem).wait()

    for load in loads[:3]:
        load.wait()
    live = jnp.where(
        lax.broadcasted_iota(jnp.int32, (1, leaf_len), 1) < sizes_ref[0], 1.0, 0.0
    ).astype(f32)

    width = 256
    groups = leaf_len // width
    order = order_ref[...]
    outer = lax.div(order, width)
    inner = order - outer * width
    with phase("onehot"):
        pick_ref[...] = jnp.where(
            lax.broadcasted_iota(jnp.int32, (width, leaf_len), 0) == inner, 1.0, 0.0
        ).astype(bf16)
    def gather(stack, pieces):
        rows = stack.shape[0] // pieces
        stacked = jnp.concatenate([stack[:, g * width : (g + 1) * width] for g in range(groups)], axis=0)
        blocks = []
        for start_col in range(0, leaf_len, width):
            cols = slice(start_col, start_col + width)
            got = dot(stacked, pick_ref[:, cols])
            total = jnp.zeros((rows, width), f32)
            for g in range(groups):
                term = None
                for piece in range(pieces):
                    base = (g * pieces + piece) * rows
                    term = got[base : base + rows] if term is None else term + got[base : base + rows]
                total = jnp.where(outer[:, cols] == g, term, total)
            blocks.append(total)
        return jnp.concatenate(blocks, axis=1)

    with phase("gather_rhs"):
        basis_ref[0] = live * gather(jnp.concatenate(split2(rhs_ref[...]), axis=0), 2)

    padded = v_all.shape[0] // 2
    used = num_levels * num_rank
    lead = 2 * nv

    def prepare(raw, both, mask=None):
        for level in range(num_levels):
            first, second = split2(raw[level] if mask is None else raw[level] * mask)
            low = level * num_rank
            both[low : low + num_rank, :] = first
            both[padded + low : padded + low + num_rank, :] = second
        if padded > used:
            both[used:padded, :] = jnp.zeros((padded - used, leaf_len), bf16)
            both[padded + used :, :] = jnp.zeros((padded - used, leaf_len), bf16)

    lane = lax.broadcasted_iota(jnp.int32, (half, lanes), 1)
    left_side = lane < num_rank

    def swap(value):
        return pltpu.roll(value, num_rank, 1)

    def send_partials(it, coef):
        for level in range(num_levels):
            block = coef[:, (level // 2) * lanes : (level // 2 + 1) * lanes]
            top, bottom = block[:half], block[half:]
            if level % 2 == 0:
                tile = jnp.where(left_side, top, swap(bottom))
            else:
                tile = jnp.where(left_side, swap(top), bottom)
            if level < levels_low:
                send_low[it, level] = tile
            else:
                for part in range(2):
                    send_high[it, part, level - levels_low] = tile[part * quarter : (part + 1) * quarter]
        for apart in reversed(range(1, size_gy)):
            send(
                send_high.at[it, lax.rem(peers[apart][1], 2)], recv_high.at[it, apart],
                part_s.at[it, 1], part_r.at[it, 1], peers[apart],
            )
        for apart in reversed(range(1, size_gy)):
            send(
                send_low.at[it, apart.bit_length() - 1], recv_low.at[it, apart],
                part_s.at[it, 0], part_r.at[it, 0], peers[apart],
            )

    def others(ref, it):
        return ref.at[it, pl.ds(1, ref.shape[1] - 1)]

    def send_nodes(it):
        with phase(f"wait_parts{it}"):
            landed(others(recv_high, it), part_r.at[it, 1])
        total = send_high[it, my_core]
        for apart in range(1, size_gy):
            total = total + recv_high[it, apart]
        send_node[it] = total
        for apart in reversed(range(1, size_gx)):
            for core in range(2):
                send(
                    send_node.at[it, apart.bit_length() - 1], recv_node.at[it, apart, my_core],
                    node_s.at[it], node_r.at[it], peers[apart * size_gy + core],
                )

    def siblings(it):
        with phase(f"wait_nodes{it}"):
            landed(others(recv_low, it), part_r.at[it, 0])
            landed(others(recv_node, it), node_r.at[it])
        tiles = []
        for count, source in ((levels_low, recv_low), (levels_high, recv_node)):
            for level in range(count):
                total = source[it, 2**level]
                for apart in range(2**level + 1, 2 ** (level + 1)):
                    total = total + source[it, apart]
                if source is recv_node:
                    total = jnp.concatenate([total[0], total[1]], axis=0)
                tiles.append(total)
        if len(tiles) % 2:
            tiles.append(jnp.zeros_like(tiles[0]))
        blocks = []
        for pair in range(len(tiles) // 2):
            even, odd = tiles[2 * pair], tiles[2 * pair + 1]
            top = jnp.where(left_side, even, swap(odd))
            bottom = jnp.where(left_side, swap(even), odd)
            blocks.append(jnp.concatenate([top, bottom], axis=0))
        return jnp.concatenate(blocks, axis=1)

    slots = lanes // nv
    row16 = lax.broadcasted_iota(jnp.int32, (nv, lanes), 0)
    slot16 = lax.broadcasted_iota(jnp.int32, (nv, lanes), 1) - row16 * slots

    def send_sums(it, values):
        block = jnp.zeros((nv, lanes), f32)
        for idx, value in enumerate(values):
            block = jnp.where(slot16 == idx, value, block)
        send_dots[it] = jnp.sum(block, axis=0, keepdims=True)
        for apart in reversed(range(1, size_all)):
            send(
                send_dots.at[it], recv_dots.at[it, apart],
                dots_s.at[it], dots_r.at[it], peers[apart],
            )

    def read_sums(it, count):
        with phase(f"wait_sums{it}"):
            landed(others(recv_dots, it), dots_r.at[it])
        terms = [send_dots[it]] + [recv_dots[it, apart] for apart in range(1, size_all)]
        while len(terms) > 1:
            terms = [terms[i] + terms[i + 1] for i in range(0, len(terms), 2)]
        return [
            jnp.sum(jnp.where(slot16 == idx, terms[0], 0.0), axis=1, keepdims=True)
            for idx in range(count)
        ]

    chunk = min(256, leaf_len)

    def doubled(value):
        first, second = split2(value)
        return jnp.concatenate([first, second], axis=0), first

    def product(both, first, hi, lo, dims=NN):
        wide = dot(both, hi, dims)
        return wide[:nv] + wide[nv:] + dot(first, lo, dims)

    def near_columns(both, first, begin, end):
        for low in range(begin, end, chunk):
            high = low + chunk
            cols = slice(low, high)
            total = product(both[:, :high], first[:, :high], near_hi[:high, cols], near_lo[:high, cols])
            if high < leaf_len:
                total = total + product(
                    both[:, high:], first[:, high:], near_hi[cols, high:], near_lo[cols, high:], NT
                )
            image_ref[:, cols] = total

    strip = min(256, chunk)

    def fill_tile(low, base):
        cols = slice(low, low + chunk)
        for start in range(base, base + chunk, strip):
            rows = slice(start, start + strip)
            square = jnp.maximum(dot(left_ref[rows, :], right_ref[:, cols]), 1e-30)
            distance = square * lax.rsqrt(square)
            value = (1.0 + distance) * jnp.exp2(distance * (-log2_e))
            hi, lo = split2(value)
            near_hi[rows, cols] = hi
            near_lo[rows, cols] = lo

    def near_tile(both, first, low, base):
        cols, rows = slice(low, low + chunk), slice(base, base + chunk)
        part = product(both[:, rows], first[:, rows], near_hi[rows, cols], near_lo[rows, cols])
        if base:
            image_ref[:, cols] += part
        else:
            image_ref[:, cols] = part
        if base < low:
            image_ref[:, rows] += product(
                both[:, cols], first[:, cols], near_hi[rows, cols], near_lo[rows, cols], NT
            )

    tiles_all = [(low, base) for low in range(0, leaf_len, chunk) for base in range(0, low + chunk, chunk)]

    def fill_near(both, first, begin, end):
        for idx in range(begin, end):
            low, base = tiles_all[idx]
            fill_tile(low, base)
            if base == low:
                cols = slice(low, low + chunk)
                vt_all[cols, :] = v_all[:, cols].T
            if idx > begin:
                near_tile(both, first, *tiles_all[idx - 1])
        near_tile(both, first, *tiles_all[end - 1])

    def prepare_points():
        for load in loads[4:7]:
            load.wait()
        with phase("gather_pos"):
            parts = [part.astype(f32) for part in split3(coords_ref[...])]
            spare = jnp.zeros((16 - 3 * num_dims, leaf_len), f32)
            got = gather(jnp.concatenate(parts + [spare], axis=0).astype(bf16), 1)
            gathered = got[:num_dims] + got[num_dims : 2 * num_dims] + got[2 * num_dims : 3 * num_dims]
            gathered = jnp.concatenate([gathered, jnp.zeros((8 - num_dims, leaf_len), f32)], axis=0)
        row8 = lax.broadcasted_iota(jnp.int32, (8, 1), 0)
        with phase("place"):
            scale = jnp.zeros((8, 1), f32)
            for dim in range(num_dims):
                scale = jnp.where(row8 == dim, inv_ref[dim] * sqrt_three, scale)
            place = (gathered - 0.5) * scale
            coarse = jnp.round(place * 4.0) * 0.25
            fine_hi, fine_lo = split2(place - coarse)
            fine_hi, fine_lo = fine_hi.astype(f32), fine_lo.astype(f32)
            fine = fine_hi + fine_lo
            whole_norm = jnp.sum(coarse * coarse, axis=0, keepdims=True)
            rest_norm = jnp.sum(fine * (2.0 * coarse + fine), axis=0, keepdims=True)
        def rows_of(values):
            block = jnp.zeros((8, leaf_len), f32)
            for idx, value in enumerate(values):
                block = jnp.where(row8 == idx, value, block)
            return block

        with phase("lr"):
            norms = [part.astype(f32) for part in split2(whole_norm)]
            rests = [part.astype(f32) for part in split3(rest_norm)]
            ones = [1.0] * 3
            pairs = [
                (-2.0 * coarse, coarse),
                (rows_of(norms + ones[:2]), rows_of(ones[:2] + norms)),
                (rows_of(rests + ones), rows_of(ones + rests)),
                (-2.0 * coarse, fine_hi),
                (-2.0 * coarse, fine_lo),
                (fine_hi, -2.0 * coarse),
                (fine_lo, -2.0 * coarse),
                (fine_hi, -2.0 * fine_hi),
                (fine_hi, -2.0 * fine_lo),
                (fine_lo, -2.0 * fine_hi),
            ]
            blank = jnp.zeros((128 - 8 * len(pairs), leaf_len), f32)
            left_ref[...] = jnp.concatenate([pair[0] for pair in pairs] + [blank], axis=0).T.astype(bf16)
            right_ref[...] = jnp.concatenate([pair[1] for pair in pairs] + [blank], axis=0).astype(bf16)

    def against(both, factors):
        size = factors.shape[1] // 2
        wide = dot(both, factors[...])
        return wide[:nv, :size] + wide[nv:, :size] + wide[:nv, size:]

    def coefs_of(name, value):
        with phase(f"coefs_{name}"):
            return product(*doubled(value), vt_all[:, :padded], vt_all[:, padded:])

    def far_of(it, coef):
        with phase(f"far{it}"):
            first, second = split2(coef)
            left = jnp.concatenate(
                [
                    jnp.concatenate([first, first], axis=1),
                    jnp.concatenate([second, jnp.zeros_like(second)], axis=1),
                ],
                axis=0,
            )
            wide = dot(left, u_all[lead:, :])
            return wide[:nv] + wide[nv:]

    def start_exchange(it, coef):
        with phase(f"send_partials{it}"):
            send_partials(it, coef)

    def operate_first(vector):
        both, first = doubled(vector)
        with phase("wait_v"):
            v_load.wait()
        with phase("prep_v"):
            prepare(v_raw, v_all)
        with phase("coef0"):
            coef = product(both, first, v_all[:padded, :], v_all[padded:, :], NT)
        with phase("wait_barrier"):
            pl.semaphore_wait(barrier, size_all - 1)
        start_exchange(0, coef)
        prepare_points()
        with phase("fillA"):
            fill_near(both, first, 0, len(tiles_all) * 5 // 9)
        send_nodes(0)
        with phase("fillB"):
            fill_near(both, first, len(tiles_all) * 5 // 9, len(tiles_all))
        u_load.wait()
        with phase("prep_u"):
            prepare(u_raw, u_all.at[pl.ds(lead, 2 * padded)], live)
        return live * image_ref[...] - vector + far_of(0, siblings(0))

    def operate_near(it, vector, relay):
        both, first = doubled(vector)
        with phase(f"nearA{it}"):
            near_columns(both, first, 0, relay)
        send_nodes(it)
        with phase(f"nearB{it}"):
            near_columns(both, first, relay, leaf_len)
        return live * image_ref[...] - vector

    def prepare_mix(near):
        with phase("mix"):
            u_all[:lead, :] = doubled(near)[0]
            wide = dot(u_all[: lead + used, :], vt_all[...])
            begin = lead + padded
            mix = wide[lead:, :padded] + wide[lead:, padded:] + dot(u_all[begin : begin + used, :], vt_all[:, :padded])
            first, second = split2(mix)
            mix_all[:used, :padded] = first
            mix_all[:used, padded:] = second
            if padded > used:
                mix_all[used:, :] = jnp.zeros((padded - used, 2 * padded), bf16)
            return wide[:nv, :padded] + wide[nv:lead, :padded] + wide[:nv, padded:]

    def lane_sum(value):
        return jnp.sum(value, axis=1, keepdims=True)

    gram = {}
    columns = []
    images = []
    beta = None
    def spread(row, vector):
        parts = jnp.concatenate(split2(vector), axis=0)
        stacked = jnp.concatenate(
            [parts * jnp.where(outer == g, 1.0, 0.0).astype(bf16) for g in range(groups)], axis=0
        )
        got = dot(stacked, pick_ref[...], NT)
        for g in range(groups):
            base = 2 * g * nv
            spread_ref[row, :, g * width : (g + 1) * width] = got[base : base + nv] + got[base + nv : base + 2 * nv]

    last_it = ITERS - 1
    raw = basis_ref[0]
    image = operate_first(raw)
    shift = 1.0 + noise_ref[0]
    coef = coefs_of("first", image)
    coefs = []
    start_exchange(1, coef)
    for it in range(ITERS):
        last = it + 1 == ITERS
        ahead = it + 2 < ITERS
        with phase(f"sums{it}"):
            values = [lane_sum(basis_ref[row] * image) for row in range(it)] + [lane_sum(raw * image)]
            values += [lane_sum(basis_ref[row] * raw) for row in range(it)] + [lane_sum(raw * raw)]
            if last:
                values.append(lane_sum(image * image))
            send_sums(it, values)
        if not last:
            near = operate_near(it + 1, image, leaf_len * (6 if it == 0 else 4) // 8)
            if ahead:
                near_coef = prepare_mix(near) if it == 0 else coefs_of(f"near{it}", near)
        else:
            for row in range(ITERS):
                with phase(f"spread{row}"):
                    spread(row, raw if row == it else basis_ref[row])
        sums = read_sums(it, len(values))
        with phase(f"scalars{it}"):
            length = jnp.sqrt(sums[2 * it + 1] + epsilon)
            inverse = 1.0 / length
            if it == 0:
                beta = length
            else:
                columns[-1].append(length)
            products = [value * inverse for value in sums[: it + 1]]
            products[it] = products[it] * inverse
            lengths = [value * inverse for value in sums[it + 1 : 2 * it + 2]]
            lengths[it] = lengths[it] * inverse
            for row in range(it + 1):
                gram[row, it] = gram[it, row] = lengths[row]
            column = [products[row] + shift * lengths[row] for row in range(it + 1)]
            moved = [column[row] - shift if row == it else column[row] for row in range(it + 1)]
            columns.append(list(column))
        if not last:
            found = siblings(it + 1)
        if ahead:
            with phase(f"coefs_next{it}"):
                coefs.append(coef * inverse)
                coef = (near_coef + against(doubled(found)[0], mix_all)) * inverse
                for row in range(it + 1):
                    coef = coef - moved[row] * coefs[row]
            start_exchange(it + 2, coef)
        if not last:
            following = near + far_of(it + 1, found)
        with phase(f"ortho{it}"):
            vector = raw * inverse
            basis_ref[it] = vector
            if last:
                rest = sums[-1] * inverse * inverse
                for row in range(it + 1):
                    inside = -2.0 * products[row]
                    for other in range(it + 1):
                        inside = inside + moved[other] * gram[row, other]
                    rest = rest + moved[row] * inside
                columns[-1].append(jnp.sqrt(jnp.maximum(rest, 0.0) + epsilon))
            else:
                images.append(image * inverse)
                raw = images[it]
                image = following * inverse
                for row in range(it + 1):
                    raw = raw - moved[row] * basis_ref[row]
                    image = image - moved[row] * images[row]
    with phase("solve"):
        weights = least_squares(columns, beta)
        weights[last_it] = weights[last_it] * inverse
        solved = weights[0] * spread_ref[0]
        for it in range(1, ITERS):
            solved = solved + weights[it] * spread_ref[it]
        out_ref[...] = solved
    for it in range(ITERS):
        landed(others(recv_high, it), part_s.at[it, 1])
        landed(others(recv_low, it), part_s.at[it, 0])
        landed(others(recv_node, it), node_s.at[it])
        landed(others(recv_dots, it), dots_s.at[it])


def per_device(
    size_gx, size_gy,
    coordinates, rhs, leaf_order, leaf_sizes, inverse_scales, noise_var, u_factors, v_factors,
):
    num_vectors, leaf_len = rhs.shape
    num_levels, num_rank = u_factors.shape[0], u_factors.shape[1]
    levels_high = size_gx.bit_length() - 1
    half, lanes = num_vectors // 2, 2 * num_rank
    padded = (num_levels + 1) // 2 * 2 * num_rank
    tile, part = (half, lanes), (half // 2, lanes)
    levels_low = size_gy.bit_length() - 1
    vmem = pl.BlockSpec(memory_space=pltpu.VMEM)
    hbm = pl.BlockSpec(memory_space=pltpu.HBM)
    dma = pltpu.SemaphoreType.DMA
    return pl.pallas_call(
        functools.partial(fused, size_gx, size_gy),
        out_shape=jax.ShapeDtypeStruct(rhs.shape, f32),
        in_specs=[hbm] * 8,
        out_specs=vmem,
        scratch_shapes=[
            pltpu.VMEM(coordinates.shape, f32),
            pltpu.VMEM(rhs.shape, f32),
            pltpu.VMEM(leaf_order.shape, jnp.int32),
            pltpu.SMEM(leaf_sizes.shape, jnp.int32),
            pltpu.SMEM(inverse_scales.shape, f32),
            pltpu.SMEM(noise_var.shape, f32),
            pltpu.VMEM((leaf_len, leaf_len), bf16),
            pltpu.VMEM((leaf_len, leaf_len), bf16),
            pltpu.VMEM((256, leaf_len), bf16),
            pltpu.VMEM((leaf_len, 128), bf16),
            pltpu.VMEM((128, leaf_len), bf16),
            pltpu.VMEM(u_factors.shape, f32),
            pltpu.VMEM(v_factors.shape, f32),
            pltpu.VMEM((2 * num_vectors + 2 * padded, leaf_len), bf16),
            pltpu.VMEM((2 * padded, leaf_len), bf16),
            pltpu.VMEM((leaf_len, 2 * padded), bf16),
            pltpu.VMEM((padded, 2 * padded), bf16),
            pltpu.VMEM((ITERS,) + rhs.shape, f32),
            pltpu.VMEM(rhs.shape, f32),
            pltpu.VMEM((ITERS, levels_low) + tile, f32),
            pltpu.VMEM((ITERS, 2, levels_high) + part, f32),
            pltpu.VMEM((ITERS, size_gy) + tile, f32),
            pltpu.VMEM((ITERS, size_gy, levels_high) + part, f32),
            pltpu.VMEM((ITERS, levels_high) + part, f32),
            pltpu.VMEM((ITERS, size_gx, 2) + part, f32),
            pltpu.VMEM((ITERS,) + rhs.shape, f32),
            pltpu.VMEM((ITERS, 1, lanes), f32),
            pltpu.VMEM((ITERS, size_gx * size_gy, 1, lanes), f32),
            dma((8,)),
            dma((ITERS, 2)),
            dma((ITERS, 2)),
            dma((ITERS,)),
            dma((ITERS,)),
            dma((ITERS,)),
            dma((ITERS,)),
        ],
        compiler_params=pltpu.CompilerParams(collective_id=0, has_side_effects=True),
        name="gmres",
    )(coordinates, rhs, leaf_order, leaf_sizes, inverse_scales, noise_var, u_factors, v_factors)


def solution(mesh):
    in_specs = (
        P(None, ("gx", "gy")),
        P(None, ("gx", "gy")),
        P(("gx", "gy"), None),
        P(("gx", "gy")),
        P(),
        P(),
        P(None, None, ("gx", "gy")),
        P(None, None, ("gx", "gy")),
    )
    out_specs = P(None, ("gx", "gy"))
    return jax.shard_map(
        functools.partial(per_device, mesh.shape["gx"], mesh.shape["gy"]),
        mesh=mesh, in_specs=in_specs, out_specs=out_specs, check_vma=False,
    )
```
